32 devices in a mesh: wide: 8 (over z, y), narrow: 4 (over x, core).
Axes of the slice: x: 2, y: 2, z: 4, core: 2. Of those that a mesh axis runs over, the one named last changes fastest.
Arguments:
- values: float32 [512, 16384], P(('wide', 'narrow')), may hold values from -200 to 200, as said below
- cloud_words: int32 [512, 512], P(('wide', 'narrow')), may hold values from -2147483648 to 2147483647, as said below
- history_len: int32 [1], replicated, may hold values from 96 to 256
- monitor_start: int32 [1], replicated, may hold values from 256 to 384
- boundary_table: int32 [512], replicated, may hold values from 500 to 2000
Outputs:
- ratio: float32 [512, 16384], P(('wide', 'narrow'))
- peak_so_far: float32 [512, 16384], P(('wide', 'narrow'))
The draws below stay inside these ranges and needn't reach their ends.
Inputs may be any that keep to these rules, and one draw needn't show every extreme that they name: `values`: values of an index series, mixed noise and a seasonal cycle of varying scale. `cloud_words`: bit b of word j in the row of date t is 1 when pixel 32 j + b is clear at date t; the first 16 dates are clear for every pixel.
All inputs are finite; a program needn't handle non-finite values.
Results may differ from the reference program's by a relative error of at most 0.0003.
Values sent between devices are 32-bit elements; how exact they have to be, the bound alone decides.
A program may use at most 64 MiB of HBM per device.

```python
import math
import jax
import jax.numpy as jnp
from jax import lax

DATES = 512
PIX_DEV = 512
PERIOD = 46
HARMONICS = 3
COLS = 8
WINDOW = 64
PIXELS = 16384


def draw_values(key, part):
    keys = jax.random.split(key, 4)
    day_float = jnp.arange(DATES, dtype=jnp.int32).astype(jnp.float32)[:, None]
    amplitude = jax.random.uniform(keys[2], (PIXELS,), jnp.float32, 0.0, 2.0)
    offset = jax.random.uniform(keys[3], (PIXELS,), jnp.float32, -math.pi, math.pi)
    seasonal = amplitude[None, :] * jnp.cos(2.0 * math.pi / PERIOD * day_float + offset[None, :])
    noise = jnp.clip(jax.random.normal(keys[0], (DATES, PIXELS), jnp.float32), -6.0, 6.0)
    scales = jnp.exp(jax.random.uniform(keys[1], (PIXELS,), jnp.float32, 0.0, math.log(10.0)))
    return scales[None, :] * (noise + seasonal)


def draw_cloud_words(key, part):
    keys = jax.random.split(jax.random.fold_in(key, 17), 2)
    lowest = jnp.iinfo(jnp.int32).min
    highest = jnp.iinfo(jnp.int32).max
    first = jax.random.randint(keys[0], (DATES, PIXELS // 32), lowest, highest, dtype=jnp.int32)
    second = jax.random.randint(keys[1], (DATES, PIXELS // 32), lowest, highest, dtype=jnp.int32)
    words = jnp.bitwise_or(first, second)
    early = (jnp.arange(DATES, dtype=jnp.int32) < 16)[:, None]
    return jnp.where(early, jnp.int32(-1), words)


def with_ends(array, stream_key, smallest, top_value):
    longest = array.shape.index(max(array.shape))
    spots = []
    for shift in (0, 1):
        where = [jax.random.randint(jax.random.fold_in(stream_key, axis), (), 0, length) for axis, length in enumerate(array.shape)]
        where[longest] = (where[longest] + shift) % array.shape[longest]
        spots.append(tuple(where))
    return array.at[spots[0]].set(smallest).at[spots[1]].set(top_value)


def setup_inputs(seed: int = 0) -> dict:
    seeds = jax.random.split(jax.random.key(seed), 6)
    return {
        "values": draw_values(jax.random.fold_in(seeds[5], 71), 0),
        "cloud_words": draw_cloud_words(jax.random.fold_in(seeds[5], 71), 0),
        "history_len": jax.random.randint(seeds[2], (1,), DATES * 3 // 16, DATES // 2 + 1).astype(jnp.int32),
        "monitor_start": jax.random.randint(seeds[3], (1,), DATES // 2, DATES * 3 // 4 + 1).astype(jnp.int32),
        "boundary_table": with_ends(jax.random.randint(seeds[4], (DATES,), 500, 2001), jax.random.fold_in(seeds[4], 1), 500, 2000).astype(jnp.int32),
    }


HIGH = lax.Precision.HIGHEST

def unpack_clear(words):
    shifts = jnp.arange(32, dtype=jnp.int32)
    flags = jnp.bitwise_and(jnp.right_shift(words[:, :, None], shifts[None, None, :]), jnp.int32(1))
    return flags.reshape(words.shape[0], words.shape[1] * 32).astype(jnp.float32)

def harmonic_design(dates):
    day_float = jnp.arange(dates, dtype=jnp.int32).astype(jnp.float32)
    columns = [jnp.ones((dates,), jnp.float32), day_float / dates]
    for harmonic in range(1, HARMONICS + 1):
        phases = 2.0 * math.pi * harmonic / PERIOD * day_float
        columns.append(jnp.cos(phases))
        columns.append(jnp.sin(phases))
    return jnp.stack(columns, axis=1)

def solve_batched(normal_mat, target):
    size_cols = normal_mat.shape[0]
    factor = [[None] * size_cols for row_idx in range(size_cols)]
    for row_idx in range(size_cols):
        for col_idx in range(row_idx + 1):
            summed = normal_mat[row_idx, col_idx]
            for mid_idx in range(col_idx):
                summed = summed - factor[row_idx][mid_idx] * factor[col_idx][mid_idx]
            if row_idx == col_idx:
                factor[row_idx][col_idx] = jnp.sqrt(summed)
            else:
                factor[row_idx][col_idx] = summed / factor[col_idx][col_idx]
    forward = []
    for row_idx in range(size_cols):
        summed = target[row_idx]
        for mid_idx in range(row_idx):
            summed = summed - factor[row_idx][mid_idx] * forward[mid_idx]
        forward.append(summed / factor[row_idx][row_idx])
    solution = [None] * size_cols
    for row_idx in reversed(range(size_cols)):
        summed = forward[row_idx]
        for mid_idx in range(row_idx + 1, size_cols):
            summed = summed - factor[mid_idx][row_idx] * solution[mid_idx]
        solution[row_idx] = summed / factor[row_idx][row_idx]
    return jnp.stack(solution, axis=0)

def fit_statistic(values, clear, history_len, monitor_start, boundary_table):
    dates = values.shape[0]
    day = jnp.arange(dates, dtype=jnp.int32)
    design = harmonic_design(dates)
    in_history = (day < history_len[0]).astype(jnp.float32)[:, None]
    weight = clear * in_history
    outer = (design[:, :, None] * design[:, None, :]).reshape(dates, COLS * COLS)
    normal_mat = jnp.dot(outer.T, weight, precision=HIGH, preferred_element_type=jnp.float32).reshape(COLS, COLS, -1)
    target = jnp.dot(design.T, weight * values, precision=HIGH, preferred_element_type=jnp.float32)
    coeffs = solve_batched(normal_mat, target)
    fitted = jnp.dot(design, coeffs, precision=HIGH, preferred_element_type=jnp.float32)
    resid = clear * (values - fitted)
    count = lax.optimization_barrier(jnp.sum(weight, axis=0))
    squares = lax.optimization_barrier(jnp.sum(weight * resid * resid, axis=0))
    sigma = jnp.sqrt(squares / (count - COLS) + 1e-06)
    lagged = day[:, None] - day[None, :]
    banded = ((lagged >= 0) & (lagged < WINDOW)).astype(jnp.float32)
    moving = jnp.dot(banded, resid, precision=HIGH, preferred_element_type=jnp.float32)
    scaled = moving / (sigma * jnp.sqrt(count))[None, :]
    bounds = boundary_table.astype(jnp.float32) * 0.001
    watching = (day >= monitor_start[0])[:, None]
    return jnp.where(watching, scaled / bounds[:, None], jnp.float32(0.0))

def reassemble(blocked):
    return blocked.transpose(1, 0, 2).reshape(DATES, -1)

def reference(values, cloud_words, history_len, monitor_start, boundary_table):
    block_count = values.shape[1] // PIX_DEV
    value_blocks = values.reshape(DATES, block_count, PIX_DEV).transpose(1, 0, 2)
    word_blocks = cloud_words.reshape(DATES, block_count, PIX_DEV // 32).transpose(1, 0, 2)

    def one_block(block_pair):
        ratio = fit_statistic(block_pair[0], unpack_clear(block_pair[1]), history_len, monitor_start, boundary_table)
        return (ratio, lax.cummax(jnp.abs(ratio), axis=0))
    ratios, peaks = lax.map(one_block, (value_blocks, word_blocks))
    return (reassemble(ratios), reassemble(peaks))
```

```python
import functools
import math

import jax
import jax.numpy as jnp
from jax import lax
from jax.experimental import pallas as pl
from jax.experimental.pallas import tpu as pltpu
import numpy as np
from jax.sharding import PartitionSpec as P

PERIOD = 46
HARMONICS = 3
COLS = 8
WINDOW = 64


HIGH = lax.Precision.HIGHEST


def unpack_clear(words):
    shifts = jnp.arange(32, dtype=jnp.int32)
    flags = jnp.bitwise_and(jnp.right_shift(words[:, :, None], shifts[None, None, :]), jnp.int32(1))
    return flags.reshape(words.shape[0], words.shape[1] * 32).astype(jnp.float32)


def harmonic_design(dates):
    day_float = jnp.arange(dates, dtype=jnp.int32).astype(jnp.float32)
    columns = [jnp.ones((dates,), jnp.float32), day_float / dates]
    for harmonic in range(1, HARMONICS + 1):
        phases = 2.0 * math.pi * harmonic / PERIOD * day_float
        columns.append(jnp.cos(phases))
        columns.append(jnp.sin(phases))
    return jnp.stack(columns, axis=1)


def solve_batched(normal_mat, target):
    size_cols = normal_mat.shape[0]
    factor = [[None] * size_cols for row_idx in range(size_cols)]
    for row_idx in range(size_cols):
        for col_idx in range(row_idx + 1):
            summed = normal_mat[row_idx, col_idx]
            for mid_idx in range(col_idx):
                summed = summed - factor[row_idx][mid_idx] * factor[col_idx][mid_idx]
            if row_idx == col_idx:
                factor[row_idx][col_idx] = jnp.sqrt(summed)
            else:
                factor[row_idx][col_idx] = summed / factor[col_idx][col_idx]
    forward = []
    for row_idx in range(size_cols):
        summed = target[row_idx]
        for mid_idx in range(row_idx):
            summed = summed - factor[row_idx][mid_idx] * forward[mid_idx]
        forward.append(summed / factor[row_idx][row_idx])
    solution = [None] * size_cols
    for row_idx in reversed(range(size_cols)):
        summed = forward[row_idx]
        for mid_idx in range(row_idx + 1, size_cols):
            summed = summed - factor[mid_idx][row_idx] * solution[mid_idx]
        solution[row_idx] = summed / factor[row_idx][row_idx]
    return jnp.stack(solution, axis=0)


def fit_statistic(values, clear, history_len, monitor_start, boundary_table):
    dates = values.shape[0]
    day = jnp.arange(dates, dtype=jnp.int32)
    design = harmonic_design(dates)
    in_history = (day < history_len[0]).astype(jnp.float32)[:, None]
    weight = clear * in_history
    outer = (design[:, :, None] * design[:, None, :]).reshape(dates, COLS * COLS)
    normal_mat = jnp.dot(
        outer.T, weight, precision=HIGH, preferred_element_type=jnp.float32
    ).reshape(COLS, COLS, -1)
    target = jnp.dot(design.T, weight * values, precision=HIGH, preferred_element_type=jnp.float32)
    coeffs = solve_batched(normal_mat, target)
    fitted = jnp.dot(design, coeffs, precision=HIGH, preferred_element_type=jnp.float32)
    resid = clear * (values - fitted)
    count = jnp.sum(weight, axis=0)
    squares = jnp.sum(weight * resid * resid, axis=0)
    sigma = jnp.sqrt(squares / (count - COLS) + 1e-06)
    lagged = day[:, None] - day[None, :]
    banded = ((lagged >= 0) & (lagged < WINDOW)).astype(jnp.float32)
    moving = jnp.dot(banded, resid, precision=HIGH, preferred_element_type=jnp.float32)
    scaled = moving / (sigma * jnp.sqrt(count))[None, :]
    bounds = boundary_table.astype(jnp.float32) * 0.001
    watching = (day >= monitor_start[0])[:, None]
    return jnp.where(watching, scaled / bounds[:, None], jnp.float32(0.0))


def per_device(values, cloud_words, history_len, monitor_start, boundary_table):
    arrived = lax.all_to_all(values, ("wide", "narrow"), split_axis=1, concat_axis=0, tiled=True)
    words = lax.all_to_all(cloud_words, ("wide", "narrow"), split_axis=1, concat_axis=0, tiled=True)
    ratio = fit_statistic(arrived, unpack_clear(words), history_len, monitor_start, boundary_table)
    rows = values.shape[0]
    blocks = ratio.reshape(ratio.shape[0] // rows, rows, ratio.shape[1])
    block_peak = lax.cummax(jnp.max(jnp.abs(blocks), axis=1), axis=0)
    earlier = jnp.concatenate([jnp.zeros_like(block_peak[:1]), block_peak[:-1]], axis=0)
    date_ratio = lax.all_to_all(ratio, ("wide", "narrow"), split_axis=0, concat_axis=1, tiled=True)
    before = lax.all_to_all(earlier, ("wide", "narrow"), split_axis=0, concat_axis=1, tiled=True)
    peak = jnp.maximum(lax.cummax(jnp.abs(date_ratio), axis=0), before)
    return (date_ratio, peak)


HISTORY_MOST = 256
MESH = pl.DeviceIdType.MESH


def host_design(dates):
    day = np.arange(dates, dtype=np.float32)
    columns = [np.ones((dates,), np.float32), (day / np.float32(dates)).astype(np.float32)]
    for harmonic in range(1, HARMONICS + 1):
        phases = (np.float32(2.0 * math.pi * harmonic / PERIOD) * day).astype(np.float64)
        columns.append(np.cos(phases).astype(np.float32))
        columns.append(np.sin(phases).astype(np.float32))
    return np.stack(columns, axis=1)


def dot_high(left, right):
    return jnp.dot(left, right, precision=HIGH, preferred_element_type=jnp.float32)


def clear_bits(words, offset, pixels):
    rows, lanes = words.shape
    parts = [((words >> (8 * k)) & 255).astype(jnp.float32).astype(jnp.bfloat16) for k in range(4)]
    stacked = jnp.concatenate(parts, axis=0)
    word_of = lax.broadcasted_iota(jnp.int32, (lanes, pixels), 1) >> 5
    spread = (lax.broadcasted_iota(jnp.int32, (lanes, pixels), 0) - offset == word_of)
    spread = spread.astype(jnp.float32).astype(jnp.bfloat16)
    wide = jnp.dot(stacked, spread, preferred_element_type=jnp.float32)
    lane = lax.broadcasted_iota(jnp.int32, (rows, pixels), 1)
    which = (lane >> 3) & 3
    byte = wide[:rows]
    for k in range(1, 4):
        byte = jnp.where(which == k, wide[k * rows : (k + 1) * rows], byte)
    return ((byte.astype(jnp.int32) >> (lane & 7)) & 1).astype(jnp.float32)


def scan_rows(array, combine, neutral):
    tiles = []
    row = lax.broadcasted_iota(jnp.int32, (8, array.shape[1]), 0)
    for at in range(0, array.shape[0], 8):
        tile = array[at : at + 8]
        for step in (1, 2, 4):
            tile = combine(tile, jnp.where(row >= step, pltpu.roll(tile, step, 0), neutral))
        if tiles:
            tile = combine(tile, tiles[-1][7:8])
        tiles.append(tile)
    return jnp.concatenate(tiles, axis=0)


def fitted(design, coeffs):
    total = design[:, 0:1] * coeffs[0:1]
    for k in range(1, COLS):
        total = total + design[:, k : k + 1] * coeffs[k : k + 1]
    return total


def solve_rows(entry, target):
    factor = [[None] * COLS for _ in range(COLS)]
    inverse = [None] * COLS
    for i in range(COLS):
        for j in range(i + 1):
            summed = entry(i, j)
            for m in range(j):
                summed = summed - factor[i][m] * factor[j][m]
            if i == j:
                inverse[i] = 1.0 / jnp.sqrt(summed)
            else:
                factor[i][j] = summed * inverse[j]
    forward = []
    for i in range(COLS):
        summed = target(i)
        for m in range(i):
            summed = summed - factor[i][m] * forward[m]
        forward.append(summed * inverse[i])
    answer = [None] * COLS
    for i in reversed(range(COLS)):
        summed = forward[i]
        for m in range(i + 1, COLS):
            summed = summed - factor[m][i] * answer[m]
        answer[i] = summed * inverse[i]
    return answer


def fused_kernel(
    narrow, chips, hist, back,
    hl_hbm, ms_hbm, b_hbm, v_hbm, w_hbm, d_hbm, ot_hbm, ratio_ref, peak_ref,
    hl_ref, ms_ref, b_ref, v_ref, w_ref, cv, cw, ccl, hv, hw, ow, tp, tb, nm, cb, cnt, sq, sb, tot, tt, sc, scb, rt, mrow, mb, dm, de, ot_ref,
    ax_s, ax_r, ha_s, ha_r, fw_s, hw_s, hw_r, ow_s, ow_r, tp_s, tp_r, cb_s, cb_r, ct_s, ct_r,
    sq_s, sq_r, tt_s, tt_r, sc_s, sc_r, mx_s, mx_r, or_s, or_r, op_s, op_r, lc,
):
    me = lax.axis_index("wide") * narrow + lax.axis_index("narrow")
    q, c = lax.div(me, 2), lax.rem(me, 2)
    rows, pixels = v_ref.shape
    half = pixels // 2
    own = half // hist
    slots = hist
    chip_rows = 2 * rows
    late = chips - hist
    is_hist = q < hist
    is_late = q >= hist

    def dev(q2, c2):
        d = 2 * q2 + c2
        return (lax.div(d, narrow), lax.rem(d, narrow))

    def remote(src, dst, ssem, rsem, q2, c2):
        return pltpu.make_async_remote_copy(
            src_ref=src, dst_ref=dst, send_sem=ssem, recv_sem=rsem,
            device_id=dev(q2, c2), device_id_type=MESH)

    def drain(ref, sem):
        pltpu.make_async_copy(ref, ref, sem).wait()

    def cols(s):
        return pl.ds(pl.multiple_of(s * own, own), own)

    mine = pl.ds(pl.multiple_of(c * rows, rows), rows)
    theirs = pl.ds(pl.multiple_of((1 - c) * rows, rows), rows)
    my_half = pl.ds(pl.multiple_of(c * half, half), half)
    other_half = pl.ds(pl.multiple_of((1 - c) * half, half), half)

    def half_col(h, s):
        return pl.ds(pl.multiple_of(h * half + s * own, own), own)

    get_w = pltpu.make_async_copy(w_hbm, w_ref, lc.at[6])
    get_v = pltpu.make_async_copy(v_hbm, v_ref, lc.at[7])
    keep_v = pltpu.make_async_copy(v_hbm.at[:, my_half], cv.at[mine, :], lc.at[0])
    keep_w = pltpu.make_async_copy(w_hbm, cw.at[mine, :], lc.at[1])
    get_scalars = [
        pltpu.make_async_copy(hl_hbm, hl_ref, lc.at[8]),
        pltpu.make_async_copy(ms_hbm, ms_ref, lc.at[9]),
        pltpu.make_async_copy(b_hbm, b_ref, lc.at[10]),
    ]
    barrier = pltpu.get_barrier_semaphore()
    devices = 2 * chips

    @pl.loop(1, devices)
    def _(k):
        to = lax.rem(me + k, devices)
        pl.semaphore_signal(
            barrier, inc=1, device_id=(lax.div(to, narrow), lax.rem(to, narrow)), device_id_type=MESH)

    get_w.start()
    get_v.start()
    keep_w.start()
    keep_v.start()
    for get in get_scalars:
        get.start()

    swap_v = remote(v_ref.at[:, other_half], cv.at[mine, :], ax_s.at[0], ax_r.at[0], q, 1 - c)
    swap_w = remote(w_ref, cw.at[mine, :], ax_s.at[1], ax_r.at[1], q, 1 - c)
    get_d = pltpu.make_async_copy(d_hbm.at[q], dm, lc.at[3])
    get_e = pltpu.make_async_copy(d_hbm.at[lax.max(q - back, 0)], de, lc.at[4])
    get_o = pltpu.make_async_copy(ot_hbm, ot_ref, lc.at[5])
    get_d.start()
    get_e.start()
    get_o.start()
    get_w.wait()
    get_v.wait()
    pl.semaphore_wait(barrier, devices - 1)
    swap_w.start()
    swap_v.start()

    def owner_block(q2, c2):
        return pl.ds(pl.multiple_of(lax.div(c2 * half + q2 * own, 32 * 128) * 128, 128), 128)

    my_dates = pl.ds(pl.multiple_of(me * rows, rows), rows)
    keep_o = pltpu.make_async_copy(w_ref.at[:, owner_block(q, c)], ow.at[my_dates, :], lc.at[2])

    def send_words(k):
        to = lax.rem(me + k, 2 * hist)
        return remote(w_ref.at[:, owner_block(lax.div(to, 2), lax.rem(to, 2))],
                      ow.at[my_dates, :], ow_s.at[0], ow_r.at[0],
                      lax.div(to, 2), lax.rem(to, 2))

    @pl.when(is_hist)
    def _():
        @pl.loop(1, 2 * hist)
        def _(k):
            send_words(k).start()
        keep_o.start()

    sends_early = jnp.logical_and(q + back >= hist, q + back < chips)
    splits = jnp.logical_and(q + back >= hist, is_hist)
    forwards = jnp.logical_and(q + 2 * back >= hist, q + back < hist)
    direct = slots // 2
    later = slots * 3 // 4

    def early_words(h):
        return remote(w_ref, hw.at[mine, :], hw_s.at[0], hw_r.at[0], q + back, h)

    def early(h, s, to):
        return remote(v_ref.at[:, half_col(h, s)], hv.at[mine, cols(s)],
                      ha_s.at[0], ha_r.at[s], to, h)

    def forward(s):
        return remote(hv.at[:, cols(s)], hv.at[:, cols(s)], fw_s.at[0], ha_r.at[s], q + 2 * back, c)

    most = slots * 5 // 8

    def start_early(when, low, high, to):
        @pl.when(when)
        def _():
            @pl.loop(low, high)
            def _(s):
                early(0, s, to).start()
                early(1, s, to).start()

    def pass_on(low, high):
        @pl.when(forwards)
        def _():
            @pl.loop(low, high)
            def _(s):
                drain(hv.at[:, cols(s)], ha_r.at[s])
                forward(s).start()

    late_sends = jnp.logical_and(is_late, sends_early)

    @pl.when(sends_early)
    def _():
        for h in range(2):
            early_words(h).start()

    start_early(splits, direct, later, q - back)
    start_early(splits, 0, direct, q + back)
    start_early(late_sends, 0, most, q + back)

    def word_block(s):
        start = c * (half // 32) + s * (own // 32)
        base = lax.div(start, 128) * 128
        return pl.ds(pl.multiple_of(base, 128), 128), start - base

    keep_w.wait()
    swap_w.wait_recv()

    @pl.loop(0, slots)
    def _(s):
        block, offset = word_block(s)
        ccl[:, cols(s)] = clear_bits(cw[:, block], offset, own)

    keep_v.wait()
    swap_v.wait_recv()
    get_d.wait()
    get_e.wait()
    get_o.wait()
    for get in get_scalars:
        get.wait()
    date = q * chip_rows + lax.broadcasted_iota(jnp.int32, (chip_rows, own), 0)

    def send_target(k):
        to = lax.rem(q + k, hist)
        return remote(tp.at[to], tb.at[q], tp_s.at[0], tp_r.at[0], to, c)

    def send_coeffs(k, base):
        return remote(cb.at[q - base], cb.at[q - base], cb_s.at[0], cb_r.at[0],
                      base + lax.rem(q - base + k, hist), c)

    relay = remote(cb.at[q], cb.at[q], cb_s.at[0], cb_r.at[1], q + hist, c)
    give_count = remote(cnt, cnt, ct_s.at[0], ct_r.at[0], q + hist, c)

    @pl.when(is_hist)
    def _():
        @pl.loop(0, slots)
        def _(s):
            weighted = jnp.where(date < hl_ref[0], ccl[:, cols(s)] * cv[:, cols(s)], 0.0)
            for k in range(COLS):
                tp[s, k : k + 1, :] = jnp.sum(weighted * dm[:, k : k + 1], axis=0, keepdims=True)

        @pl.loop(1, hist)
        def _(k):
            send_target(k).start()

        start_early(splits, later, slots, q - back)
        ratio_ref[...] = jnp.zeros_like(ratio_ref)
        peak_ref[...] = jnp.zeros_like(peak_ref)
        keep_o.wait()

        others = ow.at[pl.ds(0, (2 * hist - 1) * rows), :]
        drain(others, ow_r.at[0])

        start = c * (half // 32) + q * (own // 32)
        flags = clear_bits(ow[...], lax.rem(start, 128), own)
        day = lax.broadcasted_iota(jnp.int32, flags.shape, 0)
        nm[...] = dot_high(ot_ref[...], jnp.where(day < hl_ref[0], flags, 0.0))
        cnt[...] = nm[0:1, :]
        give_count.start()
        total = tp[q]
        pass_on(direct, later)
        drain(tb.at[pl.ds(0, hist - 1)], tp_r.at[0])

        tb[q] = total
        total = tb[0]
        for s in range(1, hist):
            total = total + tb[s]
        tb[q] = total

        def entry(i, j):
            at = i * (i + 1) // 2 + j
            return nm[at : at + 1, :]

        answer = solve_rows(entry, lambda i: tb[q, i : i + 1, :])
        for i in range(COLS):
            cb[q, i : i + 1, :] = answer[i]
        relay.start()

        @pl.loop(1, hist)
        def _(k):
            send_coeffs(k, 0).start()

        pass_on(later, slots)
        drain(cb.at[pl.ds(0, hist - 1)], cb_r.at[0])

    @pl.when(is_late)
    def _():
        drain(hw, hw_r.at[0])

        @pl.loop(0, slots)
        def _(s):
            block, offset = word_block(s)
            rt[:, cols(s)] = clear_bits(hw[:, block], offset, own)

        remote(cb.at[q - hist], cb.at[q - hist], cb_s.at[0], cb_r.at[1], q - hist, c).wait_recv()

        @pl.loop(1, hist)
        def _(k):
            send_coeffs(k, hist).start()

        start_early(late_sends, most, slots, q + back)
        drain(cb.at[pl.ds(0, hist - 1)], cb_r.at[0])

    @pl.loop(0, slots)
    def _(s):
        resid = ccl[:, cols(s)] * (cv[:, cols(s)] - fitted(dm[...], cb[s]))
        cv[:, cols(s)] = resid
        tot[0:1, cols(s)] = jnp.sum(resid, axis=0, keepdims=True)
        sq[s] = jnp.sum(jnp.where(date < hl_ref[0], resid * resid, 0.0), axis=0, keepdims=True)

    def send_total(j):
        return remote(tot, tt.at[j - 1], tt_s.at[j - 1], tt_r.at[j - 1], q + j, c)

    for j in range(1, back):
        @pl.when(jnp.logical_and(q + j >= hist, q + j < chips))
        def _():
            send_total(j).start()

    def send_squares(s):
        return remote(sq.at[s], sb.at[q], sq_s.at[0], sq_r.at[0], hist + s, c)

    @pl.when(is_hist)
    def _():
        @pl.loop(0, hist)
        def _(k):
            send_squares(lax.rem(q + k, hist)).start()

    def send_scale(k):
        return remote(sc, scb.at[q - hist], sc_s.at[0], sc_r.at[0],
                      hist + lax.rem(q - hist + k, late), c)

    def send_max(group, k):
        some = pl.ds(group * direct, direct)
        return remote(mrow.at[some], mb.at[q - hist, some], mx_s.at[k], mx_r.at[q - hist], hist + k, c)

    def ratio_out(s):
        return remote(rt.at[theirs, cols(s)], ratio_ref.at[:, half_col(c, s)], or_s.at[0], or_r.at[0], q, 1 - c)

    def peak_out(s):
        return remote(hv.at[theirs, cols(s)], peak_ref.at[:, half_col(c, s)], op_s.at[0], op_r.at[0], q, 1 - c)

    @pl.when(is_late)
    def _():
        row = lax.broadcasted_iota(jnp.int32, (chip_rows, 128), 0)
        bounds = jnp.zeros((chip_rows, 128), jnp.int32)
        for i in range(chip_rows):
            bounds = jnp.where(row == i, b_ref[q * chip_rows + i], bounds)
        over = 1.0 / (bounds[:, 0:1].astype(jnp.float32) * 0.001)

        drain(sb, sq_r.at[0])
        give_count.wait_recv()
        squares = sb[0]
        for s in range(1, hist):
            squares = squares + sb[s]
        count = cnt[...]
        sigma = jnp.sqrt(squares / (count - COLS) + 1e-06)
        scale = 1.0 / (sigma * jnp.sqrt(count))
        sc[...] = scale
        scb[q - hist] = scale

        @pl.loop(1, late)
        def _(k):
            send_scale(k).start()

        for j in range(1, back):
            send_total(j).wait_recv()

        for group in range(2):
            @pl.loop(group * direct, (group + 1) * direct)
            def _(s):
                drain(hv.at[:, cols(s)], ha_r.at[s])
                early_resid = rt[:, cols(s)] * (hv[:, cols(s)] - fitted(de[...], cb[s]))
                change = cv[:, cols(s)] - early_resid
                moving = scan_rows(change, jnp.add, 0.0) + jnp.sum(early_resid, axis=0, keepdims=True)
                for j in range(1, back):
                    moving = moving + tt[j - 1, 0:1, cols(s)]
                ratio = jnp.where(date >= ms_ref[0], moving * over, 0.0)
                rt[:, cols(s)] = ratio
                best = scan_rows(jnp.abs(ratio), jnp.maximum, 0.0)
                ccl[:, cols(s)] = best
                mrow[s] = best[chip_rows - 1 :, :]

            @pl.loop(q - hist + 1, late)
            def _(k):
                send_max(group, k).start()

        drain(scb.at[pl.ds(0, late - 1)], sc_r.at[0])

        @pl.loop(0, slots)
        def _(s):
            scaled = rt[:, cols(s)] * scb[s]
            rt[:, cols(s)] = scaled
            ratio_out(s).start()
            ratio_ref[:, half_col(c, s)] = rt[mine, cols(s)]

        @pl.loop(0, q - hist)
        def _(k):
            drain(mrow, mx_r.at[k])

        @pl.loop(0, slots)
        def _(s):
            def earlier(k, best):
                return jnp.maximum(best, mb[k, s])

            before = lax.fori_loop(0, q - hist, earlier, jnp.zeros((1, own), jnp.float32))
            hv[:, cols(s)] = jnp.maximum(ccl[:, cols(s)], before) * scb[s]
            peak_out(s).start()
            peak_ref[:, half_col(c, s)] = hv[mine, cols(s)]

        drain(ratio_ref.at[:, other_half], or_r.at[0])
        drain(peak_ref.at[:, other_half], op_r.at[0])
        drain(ratio_ref.at[:, other_half], or_s.at[0])
        drain(peak_ref.at[:, other_half], op_s.at[0])

        @pl.loop(q - hist + 1, late)
        def _(k):
            drain(mrow, mx_s.at[k])

        drain(scb.at[pl.ds(0, late - 1)], sc_s.at[0])
        drain(cb.at[pl.ds(0, hist - 1)], cb_s.at[0])

    swap_v.wait_send()
    swap_w.wait_send()

    @pl.when(is_hist)
    def _():
        drain(ow.at[pl.ds(0, (2 * hist - 1) * rows), :], ow_s.at[0])
        drain(tb.at[pl.ds(0, hist - 1)], tp_s.at[0])
        drain(cb, cb_s.at[0])
        give_count.wait_send()
        drain(sq, sq_s.at[0])

    @pl.when(sends_early)
    def _():
        drain(hw, hw_s.at[0])
        drain(v_ref, ha_s.at[0])

    @pl.when(forwards)
    def _():
        drain(hv.at[:, pl.ds(direct * own, half - direct * own)], fw_s.at[0])

    for j in range(1, back):
        @pl.when(jnp.logical_and(q + j >= hist, q + j < chips))
        def _():
            send_total(j).wait_send()


def store_kernel(ratio_ref, peak_ref, ratio_hbm, peak_hbm, sems):
    copies = [
        pltpu.make_async_copy(ratio_ref, ratio_hbm, sems.at[0]),
        pltpu.make_async_copy(peak_ref, peak_hbm, sems.at[1]),
    ]
    for copy in copies:
        copy.start()
    for copy in copies:
        copy.wait()


def fused_device(narrow, devices, values, cloud_words, history_len, monitor_start, boundary_table):
    rows, pixels = values.shape
    chips, chip_rows, half = devices // 2, 2 * rows, pixels // 2
    dates = boundary_table.shape[0]
    hist, back = HISTORY_MOST // chip_rows, WINDOW // chip_rows
    own, late = half // hist, chips - hist
    design = host_design(dates)
    lower = [(i, j) for i in range(COLS) for j in range(i + 1)]
    outer = np.zeros((40, HISTORY_MOST), np.float32)
    for at, (i, j) in enumerate(lower):
        outer[at] = design[:HISTORY_MOST, i] * design[:HISTORY_MOST, j]
    by_chip = design.reshape(chips, chip_rows, COLS)
    hbm = pl.BlockSpec(memory_space=pltpu.HBM)
    f32, i32, dma = jnp.float32, jnp.int32, pltpu.SemaphoreType.DMA
    scratch = [
        pltpu.SMEM((1,), i32),
        pltpu.SMEM((1,), i32),
        pltpu.SMEM((dates,), i32),
        pltpu.VMEM((rows, pixels), f32),
        pltpu.VMEM((rows, pixels // 32), i32),
        pltpu.VMEM((chip_rows, half), f32),
        pltpu.VMEM((chip_rows, pixels // 32), i32),
        pltpu.VMEM((chip_rows, half), f32),
        pltpu.VMEM((chip_rows, half), f32),
        pltpu.VMEM((chip_rows, pixels // 32), i32),
        pltpu.VMEM((HISTORY_MOST, 128), i32),
        pltpu.VMEM((hist, COLS, own), f32),
        pltpu.VMEM((hist, COLS, own), f32),
        pltpu.VMEM((40, own), f32),
        pltpu.VMEM((hist, COLS, own), f32),
        pltpu.VMEM((1, own), f32),
        pltpu.VMEM((hist, 1, own), f32),
        pltpu.VMEM((hist, 1, own), f32),
        pltpu.VMEM((1, half), f32),
        pltpu.VMEM((max(back - 1, 1), 1, half), f32),
        pltpu.VMEM((1, own), f32),
        pltpu.VMEM((late, 1, own), f32),
        pltpu.VMEM((chip_rows, half), f32),
        pltpu.VMEM((hist, 1, own), f32),
        pltpu.VMEM((late, hist, 1, own), f32),
        pltpu.VMEM((chip_rows, COLS), f32),
        pltpu.VMEM((chip_rows, COLS), f32),
        pltpu.VMEM((40, HISTORY_MOST), f32),
    ]
    scratch += [dma((2,)), dma((2,)), dma((1,)), dma((hist,)), dma((1,))]
    for number in (1, 1, 1):
        scratch += [dma((number,)), dma((number,))]
    scratch += [dma((1,)), dma((2,))]
    for number in (1, 1, max(back - 1, 1), 1, late, 1, 1):
        scratch += [dma((number,)), dma((number,))]
    scratch.append(dma((11,)))
    outs = pl.pallas_call(
        functools.partial(fused_kernel, narrow, chips, hist, back),
        out_shape=[pltpu.VMEM((rows, pixels), f32)] * 2,
        in_specs=[hbm] * 7,
        scratch_shapes=scratch,
        compiler_params=pltpu.CompilerParams(
            has_side_effects=True, collective_id=0, vmem_limit_bytes=67043328 - 2 * rows * pixels * 4),
    )(
        history_len, monitor_start, boundary_table, values, cloud_words,
        jnp.asarray(by_chip), jnp.asarray(outer),
    )
    return pl.pallas_call(
        store_kernel,
        out_shape=[jax.ShapeDtypeStruct((rows, pixels), f32)] * 2,
        in_specs=[pl.BlockSpec(memory_space=pltpu.VMEM)] * 2,
        out_specs=[pl.BlockSpec(memory_space=pl.ANY)] * 2,
        scratch_shapes=[dma((2,))],
        compiler_params=pltpu.CompilerParams(vmem_limit_bytes=8 * 1024 * 1024),
    )(*outs)


def fits(narrow, devices, rows, pixels):
    chip_rows = 2 * rows
    if narrow % 2 or rows % 8 or HISTORY_MOST % chip_rows or WINDOW % chip_rows:
        return False
    hist = HISTORY_MOST // chip_rows
    return devices // 2 == 2 * hist and (pixels // 2) % (hist * 128) == 0 and 128 % (pixels // 64 // hist) == 0


def solution(mesh):
    narrow = mesh.shape["narrow"]
    devices = narrow * mesh.shape["wide"]

    def per_device_any(values, *rest):
        if fits(narrow, devices, *values.shape):
            return fused_device(narrow, devices, values, *rest)
        return per_device(values, *rest)

    placed = (P(("wide", "narrow"), None), P(("wide", "narrow"), None), P(), P(), P())
    return jax.shard_map(
        per_device_any,
        mesh=mesh,
        in_specs=placed,
        out_specs=(P(("wide", "narrow"), None), P(("wide", "narrow"), None)),
        check_vma=False,
    )
```

```python
import functools
import math

import jax
import jax.numpy as jnp
from jax import lax
from jax.experimental import pallas as pl
from jax.experimental.pallas import tpu as pltpu
import numpy as np
from jax.sharding import PartitionSpec as P

PERIOD = 46
HARMONICS = 3
COLS = 8
WINDOW = 64


HIGH = lax.Precision.HIGHEST


def unpack_clear(words):
    shifts = jnp.arange(32, dtype=jnp.int32)
    flags = jnp.bitwise_and(jnp.right_shift(words[:, :, None], shifts[None, None, :]), jnp.int32(1))
    return flags.reshape(words.shape[0], words.shape[1] * 32).astype(jnp.float32)


def harmonic_design(dates):
    day_float = jnp.arange(dates, dtype=jnp.int32).astype(jnp.float32)
    columns = [jnp.ones((dates,), jnp.float32), day_float / dates]
    for harmonic in range(1, HARMONICS + 1):
        phases = 2.0 * math.pi * harmonic / PERIOD * day_float
        columns.append(jnp.cos(phases))
        columns.append(jnp.sin(phases))
    return jnp.stack(columns, axis=1)


def solve_batched(normal_mat, target):
    size_cols = normal_mat.shape[0]
    factor = [[None] * size_cols for row_idx in range(size_cols)]
    for row_idx in range(size_cols):
        for col_idx in range(row_idx + 1):
            summed = normal_mat[row_idx, col_idx]
            for mid_idx in range(col_idx):
                summed = summed - factor[row_idx][mid_idx] * factor[col_idx][mid_idx]
            if row_idx == col_idx:
                factor[row_idx][col_idx] = jnp.sqrt(summed)
            else:
                factor[row_idx][col_idx] = summed / factor[col_idx][col_idx]
    forward = []
    for row_idx in range(size_cols):
        summed = target[row_idx]
        for mid_idx in range(row_idx):
            summed = summed - factor[row_idx][mid_idx] * forward[mid_idx]
        forward.append(summed / factor[row_idx][row_idx])
    solution = [None] * size_cols
    for row_idx in reversed(range(size_cols)):
        summed = forward[row_idx]
        for mid_idx in range(row_idx + 1, size_cols):
            summed = summed - factor[mid_idx][row_idx] * solution[mid_idx]
        solution[row_idx] = summed / factor[row_idx][row_idx]
    return jnp.stack(solution, axis=0)


def fit_statistic(values, clear, history_len, monitor_start, boundary_table):
    dates = values.shape[0]
    day = jnp.arange(dates, dtype=jnp.int32)
    design = harmonic_design(dates)
    in_history = (day < history_len[0]).astype(jnp.float32)[:, None]
    weight = clear * in_history
    outer = (design[:, :, None] * design[:, None, :]).reshape(dates, COLS * COLS)
    normal_mat = jnp.dot(
        outer.T, weight, precision=HIGH, preferred_element_type=jnp.float32
    ).reshape(COLS, COLS, -1)
    target = jnp.dot(design.T, weight * values, precision=HIGH, preferred_element_type=jnp.float32)
    coeffs = solve_batched(normal_mat, target)
    fitted = jnp.dot(design, coeffs, precision=HIGH, preferred_element_type=jnp.float32)
    resid = clear * (values - fitted)
    count = jnp.sum(weight, axis=0)
    squares = jnp.sum(weight * resid * resid, axis=0)
    sigma = jnp.sqrt(squares / (count - COLS) + 1e-06)
    lagged = day[:, None] - day[None, :]
    banded = ((lagged >= 0) & (lagged < WINDOW)).astype(jnp.float32)
    moving = jnp.dot(banded, resid, precision=HIGH, preferred_element_type=jnp.float32)
    scaled = moving / (sigma * jnp.sqrt(count))[None, :]
    bounds = boundary_table.astype(jnp.float32) * 0.001
    watching = (day >= monitor_start[0])[:, None]
    return jnp.where(watching, scaled / bounds[:, None], jnp.float32(0.0))


def per_device(values, cloud_words, history_len, monitor_start, boundary_table):
    arrived = lax.all_to_all(values, ("wide", "narrow"), split_axis=1, concat_axis=0, tiled=True)
    words = lax.all_to_all(cloud_words, ("wide", "narrow"), split_axis=1, concat_axis=0, tiled=True)
    ratio = fit_statistic(arrived, unpack_clear(words), history_len, monitor_start, boundary_table)
    rows = values.shape[0]
    blocks = ratio.reshape(ratio.shape[0] // rows, rows, ratio.shape[1])
    block_peak = lax.cummax(jnp.max(jnp.abs(blocks), axis=1), axis=0)
    earlier = jnp.concatenate([jnp.zeros_like(block_peak[:1]), block_peak[:-1]], axis=0)
    date_ratio = lax.all_to_all(ratio, ("wide", "narrow"), split_axis=0, concat_axis=1, tiled=True)
    before = lax.all_to_all(earlier, ("wide", "narrow"), split_axis=0, concat_axis=1, tiled=True)
    peak = jnp.maximum(lax.cummax(jnp.abs(date_ratio), axis=0), before)
    return (date_ratio, peak)


HISTORY_MOST = 256
MESH = pl.DeviceIdType.MESH


def host_design(dates):
    day = np.arange(dates, dtype=np.float32)
    columns = [np.ones((dates,), np.float32), (day / np.float32(dates)).astype(np.float32)]
    for harmonic in range(1, HARMONICS + 1):
        phases = (np.float32(2.0 * math.pi * harmonic / PERIOD) * day).astype(np.float64)
        columns.append(np.cos(phases).astype(np.float32))
        columns.append(np.sin(phases).astype(np.float32))
    return np.stack(columns, axis=1)


def dot_high(left, right):
    return jnp.dot(left, right, precision=HIGH, preferred_element_type=jnp.float32)


def clear_bits(words, offset, pixels):
    rows, lanes = words.shape
    parts = [((words >> (8 * k)) & 255).astype(jnp.float32).astype(jnp.bfloat16) for k in range(4)]
    stacked = jnp.concatenate(parts, axis=0)
    word_of = lax.broadcasted_iota(jnp.int32, (lanes, pixels), 1) >> 5
    spread = (lax.broadcasted_iota(jnp.int32, (lanes, pixels), 0) - offset == word_of)
    spread = spread.astype(jnp.float32).astype(jnp.bfloat16)
    wide = jnp.dot(stacked, spread, preferred_element_type=jnp.float32)
    lane = lax.broadcasted_iota(jnp.int32, (rows, pixels), 1)
    which = (lane >> 3) & 3
    byte = wide[:rows]
    for k in range(1, 4):
        byte = jnp.where(which == k, wide[k * rows : (k + 1) * rows], byte)
    return ((byte.astype(jnp.int32) >> (lane & 7)) & 1).astype(jnp.float32)


def scan_rows(array, combine, neutral):
    tiles = []
    row = lax.broadcasted_iota(jnp.int32, (8, array.shape[1]), 0)
    for at in range(0, array.shape[0], 8):
        tile = array[at : at + 8]
        for step in (1, 2, 4):
            tile = combine(tile, jnp.where(row >= step, pltpu.roll(tile, step, 0), neutral))
        if tiles:
            tile = combine(tile, tiles[-1][7:8])
        tiles.append(tile)
    return jnp.concatenate(tiles, axis=0)


def fitted(design, coeffs):
    total = design[:, 0:1] * coeffs[0:1]
    for k in range(1, COLS):
        total = total + design[:, k : k + 1] * coeffs[k : k + 1]
    return total


def solve_rows(entry, target):
    factor = [[None] * COLS for _ in range(COLS)]
    inverse = [None] * COLS
    for i in range(COLS):
        for j in range(i + 1):
            summed = entry(i, j)
            for m in range(j):
                summed = summed - factor[i][m] * factor[j][m]
            if i == j:
                inverse[i] = 1.0 / jnp.sqrt(summed)
            else:
                factor[i][j] = summed * inverse[j]
    forward = []
    for i in range(COLS):
        summed = target(i)
        for m in range(i):
            summed = summed - factor[i][m] * forward[m]
        forward.append(summed * inverse[i])
    answer = [None] * COLS
    for i in reversed(range(COLS)):
        summed = forward[i]
        for m in range(i + 1, COLS):
            summed = summed - factor[m][i] * answer[m]
        answer[i] = summed * inverse[i]
    return answer


def fused_kernel(
    narrow, chips, hist, back,
    hl_hbm, ms_hbm, b_hbm, v_hbm, w_hbm, d_hbm, ot_hbm, ratio_ref, peak_ref,
    hl_ref, ms_ref, b_ref, v_ref, w_ref, cv, cw, ccl, hv, hw, ow, tp, tb, nm, cb, cnt, sq, sb, tot, te, tt, sc, scb, rt, mrow, mb, dm, de, ot_ref,
    rdy_s, ax_s, ax_r, ha_s, ha_r, fw_s, hw_s, hw_r, ow_s, ow_r, tp_s, tp_r, cb_s, cb_r, ct_s, ct_r,
    sq_s, sq_r, tt_s, tt_r, sc_s, sc_r, mx_s, mx_r, or_s, or_r, op_s, op_r, lc,
):
    me = lax.axis_index("wide") * narrow + lax.axis_index("narrow")
    q, c = lax.div(me, 2), lax.rem(me, 2)
    rows, pixels = v_ref.shape
    half = pixels // 2
    own = half // hist
    slots = hist
    chip_rows = 2 * rows
    late = chips - hist
    is_hist = q < hist
    is_late = q >= hist

    def dev(q2, c2):
        d = 2 * q2 + c2
        return (lax.div(d, narrow), lax.rem(d, narrow))

    def remote(src, dst, ssem, rsem, q2, c2):
        return pltpu.make_async_remote_copy(
            src_ref=src, dst_ref=dst, send_sem=ssem, recv_sem=rsem,
            device_id=dev(q2, c2), device_id_type=MESH)

    def drain(ref, sem):
        pltpu.make_async_copy(ref, ref, sem).wait()

    def cols(s):
        return pl.ds(pl.multiple_of(s * own, own), own)

    mine = pl.ds(pl.multiple_of(c * rows, rows), rows)
    theirs = pl.ds(pl.multiple_of((1 - c) * rows, rows), rows)
    my_half = pl.ds(pl.multiple_of(c * half, half), half)
    other_half = pl.ds(pl.multiple_of((1 - c) * half, half), half)

    def word_half(h):
        return pl.ds(pl.multiple_of(h * (half // 32), half // 32), half // 32)

    def half_col(h, s):
        return pl.ds(pl.multiple_of(h * half + s * own, own), own)

    get_w = pltpu.make_async_copy(w_hbm, w_ref, lc.at[6])
    get_v = pltpu.make_async_copy(v_hbm, v_ref, lc.at[7])
    keep_v = pltpu.make_async_copy(v_hbm.at[:, my_half], cv.at[mine, :], lc.at[0])
    keep_w = pltpu.make_async_copy(w_hbm, cw.at[mine, :], lc.at[1])
    get_scalars = [
        pltpu.make_async_copy(hl_hbm, hl_ref, lc.at[8]),
        pltpu.make_async_copy(ms_hbm, ms_ref, lc.at[9]),
        pltpu.make_async_copy(b_hbm, b_ref, lc.at[10]),
    ]
    barrier = pltpu.get_barrier_semaphore()
    rdy = rdy_s.at[0]

    def greet(to, sem):
        pl.semaphore_signal(
            sem, inc=1, device_id=(lax.div(to, narrow), lax.rem(to, narrow)), device_id_type=MESH)

    @pl.when(is_hist)
    def _():
        @pl.loop(1, 2 * hist)
        def _(k):
            greet(lax.rem(me + k, 2 * hist), barrier)
        greet(me + 2 * hist, barrier)

    @pl.when(is_late)
    def _():
        greet(2 * q + 1 - c, barrier)
        greet(2 * (q - back), barrier)
        greet(2 * (q - back) + 1, barrier)

    get_w.start()
    get_v.start()
    keep_w.start()
    keep_v.start()
    for get in get_scalars:
        get.start()

    swap_v = remote(v_ref.at[:, other_half], cv.at[mine, :], ax_s.at[0], ax_r.at[0], q, 1 - c)
    swap_w = remote(w_ref.at[:, word_half(1 - c)], cw.at[mine, word_half(1 - c)], ax_s.at[1], ax_r.at[1], q, 1 - c)
    came_w = remote(w_ref.at[:, word_half(c)], cw.at[theirs, word_half(c)], ax_s.at[1], ax_r.at[1], q, 1 - c)
    get_d = pltpu.make_async_copy(d_hbm.at[q], dm, lc.at[3])
    get_e = pltpu.make_async_copy(d_hbm.at[lax.max(q - back, 0)], de, lc.at[4])
    get_o = pltpu.make_async_copy(ot_hbm, ot_ref, lc.at[5])
    get_d.start()
    get_e.start()
    get_o.start()
    get_w.wait()
    get_v.wait()
    feeds = jnp.logical_and(q + back >= hist, q + back < chips)
    pl.semaphore_wait(barrier, jnp.where(is_hist, 2 * hist - 1, 2) + jnp.where(feeds, 2, 0))

    @pl.when(is_late)
    def _():
        greet(me - 2 * hist, rdy)

    swap_w.start()
    swap_v.start()

    def owner_block(q2, c2):
        return pl.ds(pl.multiple_of(lax.div(c2 * half + q2 * own, 32 * 128) * 128, 128), 128)

    my_dates = pl.ds(pl.multiple_of(me * rows, rows), rows)
    keep_o = pltpu.make_async_copy(w_ref.at[:, owner_block(q, c)], ow.at[my_dates, :], lc.at[2])

    def send_words(k):
        to = lax.rem(me + k, 2 * hist)
        return remote(w_ref.at[:, owner_block(lax.div(to, 2), lax.rem(to, 2))],
                      ow.at[my_dates, :], ow_s.at[0], ow_r.at[0],
                      lax.div(to, 2), lax.rem(to, 2))

    @pl.when(is_hist)
    def _():
        @pl.loop(1, 2 * hist)
        def _(k):
            send_words(k).start()
        keep_o.start()

    sends_early = jnp.logical_and(q + back >= hist, q + back < chips)
    splits = jnp.logical_and(q + back >= hist, is_hist)
    forwards = jnp.logical_and(q + 2 * back >= hist, q + back < hist)
    direct = slots // 2
    later = slots - 1

    def early_words(h):
        some = word_half(h)
        return remote(w_ref.at[:, some], hw.at[mine, some], hw_s.at[0], hw_r.at[0], q + back, h)

    def early(h, s, to):
        return remote(v_ref.at[:, half_col(h, s)], hv.at[mine, cols(s)],
                      ha_s.at[0], ha_r.at[s], to, h)

    def forward(s):
        return remote(hv.at[:, cols(s)], hv.at[:, cols(s)], fw_s.at[0], ha_r.at[s], q + 2 * back, c)

    most = slots * 5 // 8

    def start_early(when, low, high, to):
        @pl.when(when)
        def _():
            @pl.loop(low, high)
            def _(s):
                early(0, s, to).start()
                early(1, s, to).start()

    def pass_on(low, high):
        @pl.when(forwards)
        def _():
            @pl.loop(low, high)
            def _(s):
                drain(hv.at[:, cols(s)], ha_r.at[s])
                forward(s).start()

    late_sends = jnp.logical_and(is_late, sends_early)

    @pl.when(sends_early)
    def _():
        for h in range(2):
            early_words(h).start()

    start_early(splits, 0, direct, q + back)
    start_early(late_sends, 0, most, q + back)

    def word_block(s):
        start = c * (half // 32) + s * (own // 32)
        base = lax.div(start, 128) * 128
        return pl.ds(pl.multiple_of(base, 128), 128), start - base

    keep_w.wait()
    came_w.wait_recv()

    get_d.wait()
    get_e.wait()
    get_o.wait()
    for get in get_scalars:
        get.wait()
    keep_v.wait()
    swap_v.wait_recv()
    date = q * chip_rows + lax.broadcasted_iota(jnp.int32, (chip_rows, own), 0)

    def unpack(s):
        block, offset = word_block(s)
        ccl[:, cols(s)] = clear_bits(cw[:, block], offset, own)

    def send_target(to):
        return remote(tp.at[to], tb.at[q], tp_s.at[0], tp_r.at[0], to, c)

    def send_coeffs(k, base):
        return remote(cb.at[q - base], cb.at[q - base], cb_s.at[0], cb_r.at[0],
                      base + lax.rem(q - base + k, hist), c)

    relay = remote(cb.at[q], cb.at[q], cb_s.at[0], cb_r.at[1], q + hist, c)
    give_count = remote(cnt, cnt, ct_s.at[0], ct_r.at[0], q + hist, c)

    @pl.when(is_hist)
    def _():
        def part(s):
            unpack(s)
            weighted = jnp.where(date < hl_ref[0], ccl[:, cols(s)] * cv[:, cols(s)], 0.0)
            for k in range(COLS):
                tp[s, k : k + 1, :] = jnp.sum(weighted * dm[:, k : k + 1], axis=0, keepdims=True)

        part(lax.rem(q + 1, hist))
        part(lax.rem(q + 2, hist))
        pl.semaphore_wait(rdy, 1)
        send_target(lax.rem(q + 1, hist)).start()
        send_target(lax.rem(q + 2, hist)).start()

        @pl.loop(3, hist)
        def _(k):
            to = lax.rem(q + k, hist)
            part(to)
            send_target(to).start()

        part(q)

        start_early(splits, direct, later, q - back)
        ratio_ref[...] = jnp.zeros_like(ratio_ref)
        peak_ref[...] = jnp.zeros_like(peak_ref)
        keep_o.wait()

        others = ow.at[pl.ds(0, (2 * hist - 1) * rows), :]
        drain(others, ow_r.at[0])

        start = c * (half // 32) + q * (own // 32)
        flags = clear_bits(ow[...], lax.rem(start, 128), own)
        day = lax.broadcasted_iota(jnp.int32, flags.shape, 0)
        nm[...] = dot_high(ot_ref[...], jnp.where(day < hl_ref[0], flags, 0.0))
        cnt[...] = nm[0:1, :]
        give_count.start()
        total = tp[q]
        drain(tb.at[pl.ds(0, hist - 1)], tp_r.at[0])

        tb[q] = total
        total = tb[0]
        for s in range(1, hist):
            total = total + tb[s]
        tb[q] = total

        def entry(i, j):
            at = i * (i + 1) // 2 + j
            return nm[at : at + 1, :]

        answer = solve_rows(entry, lambda i: tb[q, i : i + 1, :])
        for i in range(COLS):
            cb[q, i : i + 1, :] = answer[i]
        relay.start()

        @pl.loop(1, hist)
        def _(k):
            send_coeffs(k, 0).start()

        start_early(splits, later, slots, q + back)
        pass_on(direct, later)
        drain(cb.at[pl.ds(0, hist - 1)], cb_r.at[0])

    @pl.when(is_late)
    def _():
        pl.loop(0, slots)(unpack)
        drain(hw.at[:, word_half(c)], hw_r.at[0])

        @pl.loop(0, slots)
        def _(s):
            block, offset = word_block(s)
            rt[:, cols(s)] = clear_bits(hw[:, block], offset, own)

        remote(cb.at[q - hist], cb.at[q - hist], cb_s.at[0], cb_r.at[1], q - hist, c).wait_recv()

        @pl.loop(1, hist)
        def _(k):
            send_coeffs(k, hist).start()

        start_early(late_sends, most, slots, q + back)
        drain(cb.at[pl.ds(0, hist - 1)], cb_r.at[0])

    @pl.loop(0, slots)
    def _(s):
        resid = ccl[:, cols(s)] * (cv[:, cols(s)] - fitted(dm[...], cb[s]))
        cv[:, cols(s)] = resid
        tot[0:1, cols(s)] = jnp.sum(resid, axis=0, keepdims=True)
        sq[s] = jnp.sum(jnp.where(date < hl_ref[0], resid * resid, 0.0), axis=0, keepdims=True)

    even = lax.rem(q, 2) == 0

    def group_cols(group):
        return pl.ds(group * direct * own, direct * own)

    def send_total(group, source, to):
        some = group_cols(group)
        return remote(source.at[:, some], tt.at[:, some], tt_s.at[0], tt_r.at[group], to, c)

    @pl.when(jnp.logical_and(is_late, even))
    def _():
        for group in range(2):
            send_total(group, tot, q + 1).start()

    def send_squares(s):
        return remote(sq.at[s], sb.at[q], sq_s.at[0], sq_r.at[0], hist + s, c)

    @pl.when(is_hist)
    def _():
        @pl.loop(0, hist)
        def _(k):
            send_squares(lax.rem(q + k, hist)).start()

    def send_scale(k):
        return remote(sc, scb.at[q - hist], sc_s.at[0], sc_r.at[0],
                      hist + lax.rem(q - hist + k, late), c)

    def send_max(group, k):
        some = pl.ds(group * direct, direct)
        return remote(mrow.at[some], mb.at[q - hist, some], mx_s.at[k], mx_r.at[q - hist], hist + k, c)

    def ratio_out(s):
        return remote(rt.at[theirs, cols(s)], ratio_ref.at[:, half_col(c, s)], or_s.at[0], or_r.at[0], q, 1 - c)

    def peak_out(s):
        return remote(hv.at[theirs, cols(s)], peak_ref.at[:, half_col(c, s)], op_s.at[0], op_r.at[0], q, 1 - c)

    @pl.when(is_late)
    def _():
        row = lax.broadcasted_iota(jnp.int32, (chip_rows, 128), 0)
        bounds = jnp.zeros((chip_rows, 128), jnp.int32)
        for i in range(chip_rows):
            bounds = jnp.where(row == i, b_ref[q * chip_rows + i], bounds)
        over = 1.0 / (bounds[:, 0:1].astype(jnp.float32) * 0.001)

        for group in range(2):
            @pl.loop(group * direct, (group + 1) * direct)
            def _(s):
                drain(hv.at[:, cols(s)], ha_r.at[s])
                early_resid = rt[:, cols(s)] * (hv[:, cols(s)] - fitted(de[...], cb[s]))
                change = cv[:, cols(s)] - early_resid
                early_total = jnp.sum(early_resid, axis=0, keepdims=True)
                te[0:1, cols(s)] = early_total
                rt[:, cols(s)] = scan_rows(change, jnp.add, 0.0) + early_total

            @pl.when(jnp.logical_not(even))
            def _():
                send_total(group, te, q - 1).start()

        drain(sb, sq_r.at[0])
        give_count.wait_recv()
        squares = sb[0]
        for s in range(1, hist):
            squares = squares + sb[s]
        count = cnt[...]
        sigma = jnp.sqrt(squares / (count - COLS) + 1e-06)
        scale = 1.0 / (sigma * jnp.sqrt(count))
        sc[...] = scale
        scb[q - hist] = scale

        @pl.loop(1, late)
        def _(k):
            send_scale(k).start()

        for group in range(2):
            drain(tt.at[:, group_cols(group)], tt_r.at[group])

            @pl.loop(group * direct, (group + 1) * direct)
            def _(s):
                moving = rt[:, cols(s)] + tt[0:1, cols(s)]
                ratio = jnp.where(date >= ms_ref[0], moving * over, 0.0)
                rt[:, cols(s)] = ratio
                best = scan_rows(jnp.abs(ratio), jnp.maximum, 0.0)
                ccl[:, cols(s)] = best
                mrow[s] = best[chip_rows - 1 :, :]

            @pl.loop(q - hist + 1, late)
            def _(k):
                send_max(group, k).start()

        drain(scb.at[pl.ds(0, late - 1)], sc_r.at[0])

        @pl.loop(0, slots)
        def _(s):
            scaled = rt[:, cols(s)] * scb[s]
            rt[:, cols(s)] = scaled
            ratio_out(s).start()
            ratio_ref[:, half_col(c, s)] = rt[mine, cols(s)]

        @pl.loop(0, q - hist)
        def _(k):
            drain(mrow, mx_r.at[k])

        @pl.loop(0, slots)
        def _(s):
            def earlier(k, best):
                return jnp.maximum(best, mb[k, s])

            before = lax.fori_loop(0, q - hist, earlier, jnp.zeros((1, own), jnp.float32))
            hv[:, cols(s)] = jnp.maximum(ccl[:, cols(s)], before) * scb[s]
            peak_out(s).start()
            peak_ref[:, half_col(c, s)] = hv[mine, cols(s)]

        drain(ratio_ref.at[:, other_half], or_r.at[0])
        drain(peak_ref.at[:, other_half], op_r.at[0])
        drain(ratio_ref.at[:, other_half], or_s.at[0])
        drain(peak_ref.at[:, other_half], op_s.at[0])

        @pl.loop(q - hist + 1, late)
        def _(k):
            drain(mrow, mx_s.at[k])

        drain(tot, tt_s.at[0])
        drain(scb.at[pl.ds(0, late - 1)], sc_s.at[0])
        drain(cb.at[pl.ds(0, hist - 1)], cb_s.at[0])

    swap_v.wait_send()
    swap_w.wait_send()

    @pl.when(is_hist)
    def _():
        drain(ow.at[pl.ds(0, (2 * hist - 1) * rows), :], ow_s.at[0])
        drain(tb.at[pl.ds(0, hist - 1)], tp_s.at[0])
        drain(cb, cb_s.at[0])
        give_count.wait_send()
        drain(sq, sq_s.at[0])

    @pl.when(sends_early)
    def _():
        drain(w_ref, hw_s.at[0])
        drain(v_ref, ha_s.at[0])

    @pl.when(forwards)
    def _():
        drain(hv.at[:, pl.ds(direct * own, (later - direct) * own)], fw_s.at[0])


def store_kernel(ratio_ref, peak_ref, ratio_hbm, peak_hbm, sems):
    copies = [
        pltpu.make_async_copy(ratio_ref, ratio_hbm, sems.at[0]),
        pltpu.make_async_copy(peak_ref, peak_hbm, sems.at[1]),
    ]
    for copy in copies:
        copy.start()
    for copy in copies:
        copy.wait()


def fused_device(narrow, devices, values, cloud_words, history_len, monitor_start, boundary_table):
    rows, pixels = values.shape
    chips, chip_rows, half = devices // 2, 2 * rows, pixels // 2
    dates = boundary_table.shape[0]
    hist, back = HISTORY_MOST // chip_rows, WINDOW // chip_rows
    own, late = half // hist, chips - hist
    design = host_design(dates)
    lower = [(i, j) for i in range(COLS) for j in range(i + 1)]
    outer = np.zeros((40, HISTORY_MOST), np.float32)
    for at, (i, j) in enumerate(lower):
        outer[at] = design[:HISTORY_MOST, i] * design[:HISTORY_MOST, j]
    by_chip = design.reshape(chips, chip_rows, COLS)
    hbm = pl.BlockSpec(memory_space=pltpu.HBM)
    f32, i32, dma = jnp.float32, jnp.int32, pltpu.SemaphoreType.DMA
    scratch = [
        pltpu.SMEM((1,), i32),
        pltpu.SMEM((1,), i32),
        pltpu.SMEM((dates,), i32),
        pltpu.VMEM((rows, pixels), f32),
        pltpu.VMEM((rows, pixels // 32), i32),
        pltpu.VMEM((chip_rows, half), f32),
        pltpu.VMEM((chip_rows, pixels // 32), i32),
        pltpu.VMEM((chip_rows, half), f32),
        pltpu.VMEM((chip_rows, half), f32),
        pltpu.VMEM((chip_rows, pixels // 32), i32),
        pltpu.VMEM((HISTORY_MOST, 128), i32),
        pltpu.VMEM((hist, COLS, own), f32),
        pltpu.VMEM((hist, COLS, own), f32),
        pltpu.VMEM((40, own), f32),
        pltpu.VMEM((hist, COLS, own), f32),
        pltpu.VMEM((1, own), f32),
        pltpu.VMEM((hist, 1, own), f32),
        pltpu.VMEM((hist, 1, own), f32),
        pltpu.VMEM((1, half), f32),
        pltpu.VMEM((1, half), f32),
        pltpu.VMEM((1, half), f32),
        pltpu.VMEM((1, own), f32),
        pltpu.VMEM((late, 1, own), f32),
        pltpu.VMEM((chip_rows, half), f32),
        pltpu.VMEM((hist, 1, own), f32),
        pltpu.VMEM((late, hist, 1, own), f32),
        pltpu.VMEM((chip_rows, COLS), f32),
        pltpu.VMEM((chip_rows, COLS), f32),
        pltpu.VMEM((40, HISTORY_MOST), f32),
    ]
    scratch += [pltpu.SemaphoreType.REGULAR((1,))]
    scratch += [dma((2,)), dma((2,)), dma((1,)), dma((hist,)), dma((1,))]
    for number in (1, 1, 1):
        scratch += [dma((number,)), dma((number,))]
    scratch += [dma((1,)), dma((2,))]
    for number in (1, 1):
        scratch += [dma((number,)), dma((number,))]
    scratch += [dma((1,)), dma((2,))]
    for number in (1, late, 1, 1):
        scratch += [dma((number,)), dma((number,))]
    scratch.append(dma((11,)))
    outs = pl.pallas_call(
        functools.partial(fused_kernel, narrow, chips, hist, back),
        out_shape=[pltpu.VMEM((rows, pixels), f32)] * 2,
        in_specs=[hbm] * 7,
        scratch_shapes=scratch,
        compiler_params=pltpu.CompilerParams(
            has_side_effects=True, collective_id=0, vmem_limit_bytes=67043328 - 2 * rows * pixels * 4),
    )(
        history_len, monitor_start, boundary_table, values, cloud_words,
        jnp.asarray(by_chip), jnp.asarray(outer),
    )
    return pl.pallas_call(
        store_kernel,
        out_shape=[jax.ShapeDtypeStruct((rows, pixels), f32)] * 2,
        in_specs=[pl.BlockSpec(memory_space=pltpu.VMEM)] * 2,
        out_specs=[pl.BlockSpec(memory_space=pl.ANY)] * 2,
        scratch_shapes=[dma((2,))],
        compiler_params=pltpu.CompilerParams(vmem_limit_bytes=8 * 1024 * 1024),
    )(*outs)


def fits(narrow, devices, rows, pixels):
    chip_rows = 2 * rows
    if narrow % 2 or rows % 8 or HISTORY_MOST % chip_rows or WINDOW != 2 * chip_rows:
        return False
    hist = HISTORY_MOST // chip_rows
    return devices // 2 == 2 * hist and (pixels // 2) % (hist * 128) == 0 and 128 % (pixels // 64 // hist) == 0


def solution(mesh):
    narrow = mesh.shape["narrow"]
    devices = narrow * mesh.shape["wide"]

    def per_device_any(values, *rest):
        if fits(narrow, devices, *values.shape):
            return fused_device(narrow, devices, values, *rest)
        return per_device(values, *rest)

    placed = (P(("wide", "narrow"), None), P(("wide", "narrow"), None), P(), P(), P())
    return jax.shard_map(
        per_device_any,
        mesh=mesh,
        in_specs=placed,
        out_specs=(P(("wide", "narrow"), None), P(("wide", "narrow"), None)),
        check_vma=False,
    )
```

```python
import functools
import math

import jax
import jax.numpy as jnp
from jax import lax
from jax.experimental import pallas as pl
from jax.experimental.pallas import tpu as pltpu
import numpy as np
from jax.sharding import PartitionSpec as P

PERIOD = 46
HARMONICS = 3
COLS = 8
WINDOW = 64


HIGH = lax.Precision.HIGHEST


def unpack_clear(words):
    shifts = jnp.arange(32, dtype=jnp.int32)
    flags = jnp.bitwise_and(jnp.right_shift(words[:, :, None], shifts[None, None, :]), jnp.int32(1))
    return flags.reshape(words.shape[0], words.shape[1] * 32).astype(jnp.float32)


def harmonic_design(dates):
    day_float = jnp.arange(dates, dtype=jnp.int32).astype(jnp.float32)
    columns = [jnp.ones((dates,), jnp.float32), day_float / dates]
    for harmonic in range(1, HARMONICS + 1):
        phases = 2.0 * math.pi * harmonic / PERIOD * day_float
        columns.append(jnp.cos(phases))
        columns.append(jnp.sin(phases))
    return jnp.stack(columns, axis=1)


def solve_batched(normal_mat, target):
    size_cols = normal_mat.shape[0]
    factor = [[None] * size_cols for row_idx in range(size_cols)]
    for row_idx in range(size_cols):
        for col_idx in range(row_idx + 1):
            summed = normal_mat[row_idx, col_idx]
            for mid_idx in range(col_idx):
                summed = summed - factor[row_idx][mid_idx] * factor[col_idx][mid_idx]
            if row_idx == col_idx:
                factor[row_idx][col_idx] = jnp.sqrt(summed)
            else:
                factor[row_idx][col_idx] = summed / factor[col_idx][col_idx]
    forward = []
    for row_idx in range(size_cols):
        summed = target[row_idx]
        for mid_idx in range(row_idx):
            summed = summed - factor[row_idx][mid_idx] * forward[mid_idx]
        forward.append(summed / factor[row_idx][row_idx])
    solution = [None] * size_cols
    for row_idx in reversed(range(size_cols)):
        summed = forward[row_idx]
        for mid_idx in range(row_idx + 1, size_cols):
            summed = summed - factor[mid_idx][row_idx] * solution[mid_idx]
        solution[row_idx] = summed / factor[row_idx][row_idx]
    return jnp.stack(solution, axis=0)


def fit_statistic(values, clear, history_len, monitor_start, boundary_table):
    dates = values.shape[0]
    day = jnp.arange(dates, dtype=jnp.int32)
    design = harmonic_design(dates)
    in_history = (day < history_len[0]).astype(jnp.float32)[:, None]
    weight = clear * in_history
    outer = (design[:, :, None] * design[:, None, :]).reshape(dates, COLS * COLS)
    normal_mat = jnp.dot(
        outer.T, weight, precision=HIGH, preferred_element_type=jnp.float32
    ).reshape(COLS, COLS, -1)
    target = jnp.dot(design.T, weight * values, precision=HIGH, preferred_element_type=jnp.float32)
    coeffs = solve_batched(normal_mat, target)
    fitted = jnp.dot(design, coeffs, precision=HIGH, preferred_element_type=jnp.float32)
    resid = clear * (values - fitted)
    count = jnp.sum(weight, axis=0)
    squares = jnp.sum(weight * resid * resid, axis=0)
    sigma = jnp.sqrt(squares / (count - COLS) + 1e-06)
    lagged = day[:, None] - day[None, :]
    banded = ((lagged >= 0) & (lagged < WINDOW)).astype(jnp.float32)
    moving = jnp.dot(banded, resid, precision=HIGH, preferred_element_type=jnp.float32)
    scaled = moving / (sigma * jnp.sqrt(count))[None, :]
    bounds = boundary_table.astype(jnp.float32) * 0.001
    watching = (day >= monitor_start[0])[:, None]
    return jnp.where(watching, scaled / bounds[:, None], jnp.float32(0.0))


def per_device(values, cloud_words, history_len, monitor_start, boundary_table):
    arrived = lax.all_to_all(values, ("wide", "narrow"), split_axis=1, concat_axis=0, tiled=True)
    words = lax.all_to_all(cloud_words, ("wide", "narrow"), split_axis=1, concat_axis=0, tiled=True)
    ratio = fit_statistic(arrived, unpack_clear(words), history_len, monitor_start, boundary_table)
    rows = values.shape[0]
    blocks = ratio.reshape(ratio.shape[0] // rows, rows, ratio.shape[1])
    block_peak = lax.cummax(jnp.max(jnp.abs(blocks), axis=1), axis=0)
    earlier = jnp.concatenate([jnp.zeros_like(block_peak[:1]), block_peak[:-1]], axis=0)
    date_ratio = lax.all_to_all(ratio, ("wide", "narrow"), split_axis=0, concat_axis=1, tiled=True)
    before = lax.all_to_all(earlier, ("wide", "narrow"), split_axis=0, concat_axis=1, tiled=True)
    peak = jnp.maximum(lax.cummax(jnp.abs(date_ratio), axis=0), before)
    return (date_ratio, peak)


HISTORY_MOST = 256
MESH = pl.DeviceIdType.MESH


def host_design(dates):
    day = np.arange(dates, dtype=np.float32)
    columns = [np.ones((dates,), np.float32), (day / np.float32(dates)).astype(np.float32)]
    for harmonic in range(1, HARMONICS + 1):
        phases = (np.float32(2.0 * math.pi * harmonic / PERIOD) * day).astype(np.float64)
        columns.append(np.cos(phases).astype(np.float32))
        columns.append(np.sin(phases).astype(np.float32))
    return np.stack(columns, axis=1)


def dot_high(left, right):
    return jnp.dot(left, right, precision=HIGH, preferred_element_type=jnp.float32)


def clear_bits(words, offset, pixels):
    rows, lanes = words.shape
    parts = [((words >> (8 * k)) & 255).astype(jnp.float32).astype(jnp.bfloat16) for k in range(4)]
    stacked = jnp.concatenate(parts, axis=0)
    word_of = lax.broadcasted_iota(jnp.int32, (lanes, pixels), 1) >> 5
    spread = (lax.broadcasted_iota(jnp.int32, (lanes, pixels), 0) - offset == word_of)
    spread = spread.astype(jnp.float32).astype(jnp.bfloat16)
    wide = jnp.dot(stacked, spread, preferred_element_type=jnp.float32)
    lane = lax.broadcasted_iota(jnp.int32, (rows, pixels), 1)
    which = (lane >> 3) & 3
    byte = wide[:rows]
    for k in range(1, 4):
        byte = jnp.where(which == k, wide[k * rows : (k + 1) * rows], byte)
    return ((byte.astype(jnp.int32) >> (lane & 7)) & 1).astype(jnp.float32)


def scan_rows(array, combine, neutral):
    tiles = []
    row = lax.broadcasted_iota(jnp.int32, (8, array.shape[1]), 0)
    for at in range(0, array.shape[0], 8):
        tile = array[at : at + 8]
        for step in (1, 2, 4):
            tile = combine(tile, jnp.where(row >= step, pltpu.roll(tile, step, 0), neutral))
        if tiles:
            tile = combine(tile, tiles[-1][7:8])
        tiles.append(tile)
    return jnp.concatenate(tiles, axis=0)


def fitted(design, coeffs):
    total = design[:, 0:1] * coeffs[0:1]
    for k in range(1, COLS):
        total = total + design[:, k : k + 1] * coeffs[k : k + 1]
    return total


def solve_rows(entry, target):
    factor = [[None] * COLS for _ in range(COLS)]
    inverse = [None] * COLS
    for i in range(COLS):
        for j in range(i + 1):
            summed = entry(i, j)
            for m in range(j):
                summed = summed - factor[i][m] * factor[j][m]
            if i == j:
                inverse[i] = 1.0 / jnp.sqrt(summed)
            else:
                factor[i][j] = summed * inverse[j]
    forward = []
    for i in range(COLS):
        summed = target(i)
        for m in range(i):
            summed = summed - factor[i][m] * forward[m]
        forward.append(summed * inverse[i])
    answer = [None] * COLS
    for i in reversed(range(COLS)):
        summed = forward[i]
        for m in range(i + 1, COLS):
            summed = summed - factor[m][i] * answer[m]
        answer[i] = summed * inverse[i]
    return answer


def fused_kernel(
    narrow, chips, hist, back,
    hl_hbm, ms_hbm, b_hbm, v_hbm, w_hbm, d_hbm, ot_hbm, ratio_ref, peak_ref,
    hl_ref, ms_ref, b_ref, v_ref, w_ref, fw, cv, cw, ccl, hv, hw, ow, tp, tb, nm, cb, cnt, sq, sb, tot, tt, sc, scb, rt, mrow, mb, dm, de, ot_ref,
    rdy_s, ax_s, ax_r, ha_s, ha_r, fw_s, fw_r, hw_s, hw_r, ow_s, ow_r, tp_s, tp_r, cb_s, cb_r, ct_s, ct_r,
    sq_s, sq_r, tt_s, tt_r, sc_s, sc_r, mx_s, mx_r, or_s, or_r, op_s, op_r, lc,
):
    me = lax.axis_index("wide") * narrow + lax.axis_index("narrow")
    q, c = lax.div(me, 2), lax.rem(me, 2)
    rows, pixels = v_ref.shape
    half = pixels // 2
    own = half // hist
    slots = hist
    chip_rows = 2 * rows
    late = chips - hist
    is_hist = q < hist
    is_late = q >= hist

    def dev(q2, c2):
        d = 2 * q2 + c2
        return (lax.div(d, narrow), lax.rem(d, narrow))

    def remote(src, dst, ssem, rsem, q2, c2):
        return pltpu.make_async_remote_copy(
            src_ref=src, dst_ref=dst, send_sem=ssem, recv_sem=rsem,
            device_id=dev(q2, c2), device_id_type=MESH)

    def drain(ref, sem):
        pltpu.make_async_copy(ref, ref, sem).wait()

    def cols(s):
        return pl.ds(pl.multiple_of(s * own, own), own)

    mine = pl.ds(pl.multiple_of(c * rows, rows), rows)
    theirs = pl.ds(pl.multiple_of((1 - c) * rows, rows), rows)
    my_half = pl.ds(pl.multiple_of(c * half, half), half)
    other_half = pl.ds(pl.multiple_of((1 - c) * half, half), half)

    def word_half(h):
        return pl.ds(pl.multiple_of(h * (half // 32), half // 32), half // 32)

    def half_col(h, s):
        return pl.ds(pl.multiple_of(h * half + s * own, own), own)

    get_w = pltpu.make_async_copy(w_hbm, w_ref, lc.at[6])
    get_v = pltpu.make_async_copy(v_hbm, v_ref, lc.at[7])
    keep_v = pltpu.make_async_copy(v_hbm.at[:, my_half], cv.at[mine, :], lc.at[0])
    keep_w = pltpu.make_async_copy(w_hbm, cw.at[mine, :], lc.at[1])
    get_scalars = [
        pltpu.make_async_copy(hl_hbm, hl_ref, lc.at[8]),
        pltpu.make_async_copy(ms_hbm, ms_ref, lc.at[9]),
        pltpu.make_async_copy(b_hbm, b_ref, lc.at[10]),
    ]
    barrier = pltpu.get_barrier_semaphore()
    rdy = rdy_s.at[0]

    def greet(to, sem):
        pl.semaphore_signal(
            sem, inc=1, device_id=(lax.div(to, narrow), lax.rem(to, narrow)), device_id_type=MESH)

    @pl.when(is_hist)
    def _():
        @pl.loop(1, 2 * hist)
        def _(k):
            greet(lax.rem(me + k, 2 * hist), barrier)
        greet(me + 2 * hist, barrier)

    @pl.when(is_late)
    def _():
        greet(2 * q + 1 - c, barrier)
        greet(2 * (q - back), barrier)
        greet(2 * (q - back) + 1, barrier)

    late_splits = jnp.logical_and(q >= hist + back, q < hist + 2 * back)
    late_passes = jnp.logical_and(q >= hist, q < hist + back)

    @pl.when(late_passes)
    def _():
        greet(2 * (q + back), barrier)
        greet(2 * (q + back) + 1, barrier)

    get_w.start()
    get_v.start()
    keep_w.start()
    keep_v.start()
    for get in get_scalars:
        get.start()

    swap_v = remote(v_ref.at[:, other_half], cv.at[mine, :], ax_s.at[0], ax_r.at[0], q, 1 - c)
    swap_w = remote(w_ref.at[:, word_half(1 - c)], cw.at[mine, word_half(1 - c)], ax_s.at[1], ax_r.at[1], q, 1 - c)
    came_w = remote(w_ref.at[:, word_half(c)], cw.at[theirs, word_half(c)], ax_s.at[1], ax_r.at[1], q, 1 - c)
    get_d = pltpu.make_async_copy(d_hbm.at[q], dm, lc.at[3])
    get_e = pltpu.make_async_copy(d_hbm.at[lax.max(q - back, 0)], de, lc.at[4])
    get_o = pltpu.make_async_copy(ot_hbm, ot_ref, lc.at[5])
    get_d.start()
    get_e.start()
    get_o.start()
    get_w.wait()
    get_v.wait()
    feeds = jnp.logical_and(q + back >= hist, q + back < chips)
    greeted = jnp.where(is_hist, 2 * hist - 1, 2) + jnp.where(feeds, 2, 0) + jnp.where(late_splits, 2, 0)
    pl.semaphore_wait(barrier, greeted)

    @pl.when(is_late)
    def _():
        greet(me - 2 * hist, rdy)

    swap_w.start()
    swap_v.start()

    def owner_block(q2, c2):
        return pl.ds(pl.multiple_of(lax.div(c2 * half + q2 * own, 32 * 128) * 128, 128), 128)

    my_dates = pl.ds(pl.multiple_of(me * rows, rows), rows)
    keep_o = pltpu.make_async_copy(w_ref.at[:, owner_block(q, c)], ow.at[my_dates, :], lc.at[2])

    def send_words(k):
        to = lax.rem(me + k, 2 * hist)
        return remote(w_ref.at[:, owner_block(lax.div(to, 2), lax.rem(to, 2))],
                      ow.at[my_dates, :], ow_s.at[0], ow_r.at[0],
                      lax.div(to, 2), lax.rem(to, 2))

    @pl.when(is_hist)
    def _():
        @pl.loop(1, 2 * hist)
        def _(k):
            send_words(k).start()
        keep_o.start()

    sends_early = jnp.logical_and(q + back >= hist, q + back < chips)
    splits = jnp.logical_and(q + back >= hist, is_hist)
    forwards = jnp.logical_and(q + 2 * back >= hist, q + back < hist)
    direct = slots * 3 // 8
    later = slots - 1
    middle = (direct + later) // 2

    def early_words(h):
        some = word_half(h)
        return remote(w_ref.at[:, some], hw.at[mine, some], hw_s.at[0], hw_r.at[0], q + back, h)

    def early(h, s, to):
        return remote(v_ref.at[:, half_col(h, s)], hv.at[mine, cols(s)],
                      ha_s.at[0], ha_r.at[s], to, h)

    def forward(s):
        return remote(hv.at[:, cols(s)], hv.at[:, cols(s)], fw_s.at[0], ha_r.at[s], q + 2 * back, c)

    most = slots // 2
    first = slots * 3 // 4

    def start_early(when, low, high, to):
        @pl.when(when)
        def _():
            @pl.loop(low, high)
            def _(s):
                early(0, s, to).start()
                early(1, s, to).start()

    def pass_on(low, high):
        @pl.when(forwards)
        def _():
            @pl.loop(low, high)
            def _(s):
                drain(hv.at[:, cols(s)], ha_r.at[s])
                forward(s).start()

    late_sends = jnp.logical_and(is_late, sends_early)
    late_direct = jnp.logical_and(late_sends, jnp.logical_not(late_splits))
    via = 1

    def early_via(h, i):
        return remote(v_ref.at[:, half_col(h, most + i)], fw.at[mine, cols(i)], ha_s.at[0], fw_r.at[i], q - back, h)

    def late_forward(i):
        @pl.when(late_passes)
        def _():
            drain(fw.at[:, cols(i)], fw_r.at[i])
            remote(fw.at[:, cols(i)], hv.at[:, cols(most + i)], fw_s.at[0], ha_r.at[most + i], q + 2 * back, c).start()

    @pl.when(sends_early)
    def _():
        for h in range(2):
            early_words(h).start()

    start_early(splits, 0, direct, q + back)
    start_early(late_sends, 0, most, q + back)

    def word_block(s):
        start = c * (half // 32) + s * (own // 32)
        base = lax.div(start, 128) * 128
        return pl.ds(pl.multiple_of(base, 128), 128), start - base

    keep_w.wait()
    came_w.wait_recv()

    get_d.wait()
    get_e.wait()
    get_o.wait()
    for get in get_scalars:
        get.wait()
    keep_v.wait()
    swap_v.wait_recv()
    date = q * chip_rows + lax.broadcasted_iota(jnp.int32, (chip_rows, own), 0)

    def unpack(s):
        block, offset = word_block(s)
        ccl[:, cols(s)] = clear_bits(cw[:, block], offset, own)

    def send_target(to):
        return remote(tp.at[to], tb.at[q], tp_s.at[0], tp_r.at[0], to, c)

    columns = late // 2

    def send_coeffs(k):
        return remote(cb.at[q], cb.at[q], cb_s.at[0], cb_r.at[0], lax.rem(q + k, hist), c)

    def column_coeffs(k):
        return remote(cb.at[q - hist], cb.at[q - hist], cb_s.at[0], cb_r.at[1 + k],
                      hist + lax.rem(q - hist + 2 * k, late), c)

    def cross_coeffs(s):
        return remote(cb.at[s], cb.at[s], cb_s.at[0], cb_r.at[0], q + 1 - 2 * lax.rem(q, 2), c)

    relay = remote(cb.at[q], cb.at[q], cb_s.at[0], cb_r.at[1], q + hist, c)
    give_count = remote(cnt, cnt, ct_s.at[0], ct_r.at[0], q + hist, c)

    @pl.when(is_hist)
    def _():
        def part(s):
            unpack(s)
            weighted = jnp.where(date < hl_ref[0], ccl[:, cols(s)] * cv[:, cols(s)], 0.0)
            for k in range(COLS):
                tp[s, k : k + 1, :] = jnp.sum(weighted * dm[:, k : k + 1], axis=0, keepdims=True)

        part(lax.rem(q + 1, hist))
        part(lax.rem(q + 2, hist))
        pl.semaphore_wait(rdy, 1)
        send_target(lax.rem(q + 1, hist)).start()
        send_target(lax.rem(q + 2, hist)).start()

        @pl.loop(3, hist)
        def _(k):
            to = lax.rem(q + k, hist)
            part(to)
            send_target(to).start()

        part(q)

        start_early(splits, direct, middle, q - back)
        ratio_ref[...] = jnp.zeros_like(ratio_ref)
        peak_ref[...] = jnp.zeros_like(peak_ref)
        keep_o.wait()

        others = ow.at[pl.ds(0, (2 * hist - 1) * rows), :]
        drain(others, ow_r.at[0])

        start = c * (half // 32) + q * (own // 32)
        flags = clear_bits(ow[...], lax.rem(start, 128), own)
        day = lax.broadcasted_iota(jnp.int32, flags.shape, 0)
        nm[...] = dot_high(ot_ref[...], jnp.where(day < hl_ref[0], flags, 0.0))
        cnt[...] = nm[0:1, :]
        give_count.start()
        total = tp[q]
        drain(tb.at[pl.ds(0, hist - 1)], tp_r.at[0])

        tb[q] = total
        total = tb[0]
        for s in range(1, hist):
            total = total + tb[s]
        tb[q] = total

        def entry(i, j):
            at = i * (i + 1) // 2 + j
            return nm[at : at + 1, :]

        answer = solve_rows(entry, lambda i: tb[q, i : i + 1, :])
        for i in range(COLS):
            cb[q, i : i + 1, :] = answer[i]
        relay.start()

        @pl.loop(1, hist)
        def _(k):
            send_coeffs(k).start()

        start_early(splits, middle, later, q - back)
        start_early(splits, later, slots, q + back)
        pass_on(direct, middle)
        drain(cb.at[pl.ds(0, hist - 1)], cb_r.at[0])

    @pl.when(is_late)
    def _():
        pl.loop(0, slots)(unpack)
        drain(hw.at[:, word_half(c)], hw_r.at[0])

        @pl.loop(0, slots)
        def _(s):
            block, offset = word_block(s)
            rt[:, cols(s)] = clear_bits(hw[:, block], offset, own)

        remote(cb.at[q - hist], cb.at[q - hist], cb_s.at[0], cb_r.at[1], q - hist, c).wait_recv()

        @pl.loop(1, columns)
        def _(k):
            column_coeffs(k).start()

        cross_coeffs(q - hist).start()
        start_early(late_direct, most, most + via, q + back)
        start_early(late_sends, most + via, slots - 1, q + back)

        @pl.when(late_splits)
        def _():
            for i in range(via):
                for h in range(2):
                    early_via(h, i).start()

        @pl.loop(1, columns)
        def _(k):
            from_column = lax.rem(q - hist + late - 2 * k, late)
            drain(cb.at[from_column], cb_r.at[1 + k])
            cross_coeffs(from_column).start()

        late_forward(0)
        drain(cb.at[pl.ds(0, columns)], cb_r.at[0])

    @pl.loop(0, slots)
    def _(s):
        resid = ccl[:, cols(s)] * (cv[:, cols(s)] - fitted(dm[...], cb[s]))
        cv[:, cols(s)] = resid
        tot[0:1, cols(s)] = jnp.sum(resid, axis=0, keepdims=True)
        sq[s] = jnp.sum(jnp.where(date < hl_ref[0], resid * resid, 0.0), axis=0, keepdims=True)

    totals = jnp.logical_and(q + 1 >= hist, q + 1 < chips)
    send_total = remote(tot, tt, tt_s.at[0], tt_r.at[0], q + 1, c)

    @pl.when(totals)
    def _():
        send_total.start()

    start_early(late_sends, slots - 1, slots, q + back)

    def send_squares(s):
        return remote(sq.at[s], sb.at[q], sq_s.at[0], sq_r.at[0], hist + s, c)

    @pl.when(is_hist)
    def _():
        @pl.loop(0, hist)
        def _(k):
            send_squares(lax.rem(q + k, hist)).start()

        pass_on(middle, later)

    def send_scale(k):
        return remote(sc, scb.at[q - hist], sc_s.at[0], sc_r.at[0],
                      hist + lax.rem(q - hist + k, late), c)

    def send_max(group, k):
        some = pl.ds(0, first) if group == 0 else pl.ds(first, slots - first)
        return remote(mrow.at[some], mb.at[q - hist, some], mx_s.at[k], mx_r.at[q - hist], hist + k, c)

    def ratio_out(s):
        return remote(rt.at[theirs, cols(s)], ratio_ref.at[:, half_col(c, s)], or_s.at[0], or_r.at[0], q, 1 - c)

    def peak_out(s):
        return remote(hv.at[theirs, cols(s)], peak_ref.at[:, half_col(c, s)], op_s.at[0], op_r.at[0], q, 1 - c)

    @pl.when(is_late)
    def _():
        row = lax.broadcasted_iota(jnp.int32, (chip_rows, 128), 0)
        bounds = jnp.zeros((chip_rows, 128), jnp.int32)
        for i in range(chip_rows):
            bounds = jnp.where(row == i, b_ref[q * chip_rows + i], bounds)
        over = 1.0 / (bounds[:, 0:1].astype(jnp.float32) * 0.001)

        def window(s):
            drain(hv.at[:, cols(s)], ha_r.at[s])
            early_resid = rt[:, cols(s)] * (hv[:, cols(s)] - fitted(de[...], cb[s]))
            change = cv[:, cols(s)] - early_resid
            return scan_rows(change, jnp.add, 0.0) + jnp.sum(early_resid, axis=0, keepdims=True)

        def statistic(s, partial):
            moving = partial + tt[0:1, cols(s)]
            ratio = jnp.where(date >= ms_ref[0], moving * over, 0.0)
            rt[:, cols(s)] = ratio
            best = scan_rows(jnp.abs(ratio), jnp.maximum, 0.0)
            ccl[:, cols(s)] = best
            mrow[s] = best[chip_rows - 1 :, :]

        def send_maxima(group):
            @pl.loop(q - hist + 1, late)
            def _(k):
                send_max(group, k).start()

        @pl.loop(0, first)
        def _(s):
            rt[:, cols(s)] = window(s)

        drain(sb, sq_r.at[0])
        give_count.wait_recv()
        squares = sb[0]
        for s in range(1, hist):
            squares = squares + sb[s]
        count = cnt[...]
        sigma = jnp.sqrt(squares / (count - COLS) + 1e-06)
        scale = 1.0 / (sigma * jnp.sqrt(count))
        sc[...] = scale
        scb[q - hist] = scale

        @pl.loop(1, late)
        def _(k):
            send_scale(k).start()

        send_total.wait_recv()

        @pl.loop(0, first)
        def _(s):
            statistic(s, rt[:, cols(s)])

        send_maxima(0)

        @pl.loop(first, slots)
        def _(s):
            statistic(s, window(s))

        send_maxima(1)
        drain(scb.at[pl.ds(0, late - 1)], sc_r.at[0])

        @pl.loop(0, slots)
        def _(s):
            scaled = rt[:, cols(s)] * scb[s]
            rt[:, cols(s)] = scaled
            ratio_out(s).start()
            ratio_ref[:, half_col(c, s)] = rt[mine, cols(s)]

        @pl.loop(0, q - hist)
        def _(k):
            drain(mrow, mx_r.at[k])

        @pl.loop(0, slots)
        def _(s):
            def earlier(k, best):
                return jnp.maximum(best, mb[k, s])

            before = lax.fori_loop(0, q - hist, earlier, jnp.zeros((1, own), jnp.float32))
            hv[:, cols(s)] = jnp.maximum(ccl[:, cols(s)], before) * scb[s]
            peak_out(s).start()
            peak_ref[:, half_col(c, s)] = hv[mine, cols(s)]

        drain(ratio_ref.at[:, other_half], or_r.at[0])
        drain(peak_ref.at[:, other_half], op_r.at[0])
        drain(ratio_ref.at[:, other_half], or_s.at[0])
        drain(peak_ref.at[:, other_half], op_s.at[0])

        @pl.loop(q - hist + 1, late)
        def _(k):
            drain(mrow, mx_s.at[k])

        drain(scb.at[pl.ds(0, late - 1)], sc_s.at[0])
        drain(cb.at[pl.ds(0, hist - 1)], cb_s.at[0])

    swap_v.wait_send()
    swap_w.wait_send()

    @pl.when(is_hist)
    def _():
        drain(ow.at[pl.ds(0, (2 * hist - 1) * rows), :], ow_s.at[0])
        drain(tb.at[pl.ds(0, hist - 1)], tp_s.at[0])
        drain(cb, cb_s.at[0])
        give_count.wait_send()
        drain(sq, sq_s.at[0])

    @pl.when(totals)
    def _():
        send_total.wait_send()

    @pl.when(sends_early)
    def _():
        drain(w_ref, hw_s.at[0])
        drain(v_ref, ha_s.at[0])

    @pl.when(late_passes)
    def _():
        drain(fw, fw_s.at[0])

    @pl.when(forwards)
    def _():
        drain(hv.at[:, pl.ds(direct * own, (later - direct) * own)], fw_s.at[0])


def store_kernel(ratio_ref, peak_ref, ratio_hbm, peak_hbm, sems):
    copies = [
        pltpu.make_async_copy(ratio_ref, ratio_hbm, sems.at[0]),
        pltpu.make_async_copy(peak_ref, peak_hbm, sems.at[1]),
    ]
    for copy in copies:
        copy.start()
    for copy in copies:
        copy.wait()


def fused_device(narrow, devices, values, cloud_words, history_len, monitor_start, boundary_table):
    rows, pixels = values.shape
    chips, chip_rows, half = devices // 2, 2 * rows, pixels // 2
    dates = boundary_table.shape[0]
    hist, back = HISTORY_MOST // chip_rows, WINDOW // chip_rows
    own, late = half // hist, chips - hist
    design = host_design(dates)
    lower = [(i, j) for i in range(COLS) for j in range(i + 1)]
    outer = np.zeros((40, HISTORY_MOST), np.float32)
    for at, (i, j) in enumerate(lower):
        outer[at] = design[:HISTORY_MOST, i] * design[:HISTORY_MOST, j]
    by_chip = design.reshape(chips, chip_rows, COLS)
    hbm = pl.BlockSpec(memory_space=pltpu.HBM)
    f32, i32, dma = jnp.float32, jnp.int32, pltpu.SemaphoreType.DMA
    scratch = [
        pltpu.SMEM((1,), i32),
        pltpu.SMEM((1,), i32),
        pltpu.SMEM((dates,), i32),
        pltpu.VMEM((rows, pixels), f32),
        pltpu.VMEM((rows, pixels // 32), i32),
        pltpu.VMEM((chip_rows, own), f32),
        pltpu.VMEM((chip_rows, half), f32),
        pltpu.VMEM((chip_rows, pixels // 32), i32),
        pltpu.VMEM((chip_rows, half), f32),
        pltpu.VMEM((chip_rows, half), f32),
        pltpu.VMEM((chip_rows, pixels // 32), i32),
        pltpu.VMEM((HISTORY_MOST, 128), i32),
        pltpu.VMEM((hist, COLS, own), f32),
        pltpu.VMEM((hist, COLS, own), f32),
        pltpu.VMEM((40, own), f32),
        pltpu.VMEM((hist, COLS, own), f32),
        pltpu.VMEM((1, own), f32),
        pltpu.VMEM((hist, 1, own), f32),
        pltpu.VMEM((hist, 1, own), f32),
        pltpu.VMEM((1, half), f32),
        pltpu.VMEM((1, half), f32),
        pltpu.VMEM((1, own), f32),
        pltpu.VMEM((late, 1, own), f32),
        pltpu.VMEM((chip_rows, half), f32),
        pltpu.VMEM((hist, 1, own), f32),
        pltpu.VMEM((late, hist, 1, own), f32),
        pltpu.VMEM((chip_rows, COLS), f32),
        pltpu.VMEM((chip_rows, COLS), f32),
        pltpu.VMEM((40, HISTORY_MOST), f32),
    ]
    scratch += [pltpu.SemaphoreType.REGULAR((1,))]
    scratch += [dma((2,)), dma((2,)), dma((1,)), dma((hist,)), dma((1,)), dma((1,))]
    for number in (1, 1, 1):
        scratch += [dma((number,)), dma((number,))]
    scratch += [dma((1,)), dma((1 + late // 2,))]
    for number in (1, 1):
        scratch += [dma((number,)), dma((number,))]
    scratch += [dma((1,)), dma((1,))]
    for number in (1, late, 1, 1):
        scratch += [dma((number,)), dma((number,))]
    scratch.append(dma((11,)))
    outs = pl.pallas_call(
        functools.partial(fused_kernel, narrow, chips, hist, back),
        out_shape=[pltpu.VMEM((rows, pixels), f32)] * 2,
        in_specs=[hbm] * 7,
        scratch_shapes=scratch,
        compiler_params=pltpu.CompilerParams(
            has_side_effects=True, collective_id=0, vmem_limit_bytes=67043328 - 2 * rows * pixels * 4),
    )(
        history_len, monitor_start, boundary_table, values, cloud_words,
        jnp.asarray(by_chip), jnp.asarray(outer),
    )
    return pl.pallas_call(
        store_kernel,
        out_shape=[jax.ShapeDtypeStruct((rows, pixels), f32)] * 2,
        in_specs=[pl.BlockSpec(memory_space=pltpu.VMEM)] * 2,
        out_specs=[pl.BlockSpec(memory_space=pl.ANY)] * 2,
        scratch_shapes=[dma((2,))],
        compiler_params=pltpu.CompilerParams(vmem_limit_bytes=8 * 1024 * 1024),
    )(*outs)


def fits(narrow, devices, rows, pixels):
    chip_rows = 2 * rows
    if narrow % 2 or rows % 8 or HISTORY_MOST % chip_rows or WINDOW != 2 * chip_rows:
        return False
    hist = HISTORY_MOST // chip_rows
    return devices // 2 == 2 * hist and (pixels // 2) % (hist * 128) == 0 and 128 % (pixels // 64 // hist) == 0


def solution(mesh):
    narrow = mesh.shape["narrow"]
    devices = narrow * mesh.shape["wide"]

    def per_device_any(values, *rest):
        if fits(narrow, devices, *values.shape):
            return fused_device(narrow, devices, values, *rest)
        return per_device(values, *rest)

    placed = (P(("wide", "narrow"), None), P(("wide", "narrow"), None), P(), P(), P())
    return jax.shard_map(
        per_device_any,
        mesh=mesh,
        in_specs=placed,
        out_specs=(P(("wide", "narrow"), None), P(("wide", "narrow"), None)),
        check_vma=False,
    )
```

```python
import functools
import math

import jax
import jax.numpy as jnp
from jax import lax
from jax.experimental import pallas as pl
from jax.experimental.pallas import tpu as pltpu
import numpy as np
from jax.sharding import PartitionSpec as P

PERIOD = 46
HARMONICS = 3
COLS = 8
WINDOW = 64


HIGH = lax.Precision.HIGHEST


def unpack_clear(words):
    shifts = jnp.arange(32, dtype=jnp.int32)
    flags = jnp.bitwise_and(jnp.right_shift(words[:, :, None], shifts[None, None, :]), jnp.int32(1))
    return flags.reshape(words.shape[0], words.shape[1] * 32).astype(jnp.float32)


def harmonic_design(dates):
    day_float = jnp.arange(dates, dtype=jnp.int32).astype(jnp.float32)
    columns = [jnp.ones((dates,), jnp.float32), day_float / dates]
    for harmonic in range(1, HARMONICS + 1):
        phases = 2.0 * math.pi * harmonic / PERIOD * day_float
        columns.append(jnp.cos(phases))
        columns.append(jnp.sin(phases))
    return jnp.stack(columns, axis=1)


def solve_batched(normal_mat, target):
    size_cols = normal_mat.shape[0]
    factor = [[None] * size_cols for row_idx in range(size_cols)]
    for row_idx in range(size_cols):
        for col_idx in range(row_idx + 1):
            summed = normal_mat[row_idx, col_idx]
            for mid_idx in range(col_idx):
                summed = summed - factor[row_idx][mid_idx] * factor[col_idx][mid_idx]
            if row_idx == col_idx:
                factor[row_idx][col_idx] = jnp.sqrt(summed)
            else:
                factor[row_idx][col_idx] = summed / factor[col_idx][col_idx]
    forward = []
    for row_idx in range(size_cols):
        summed = target[row_idx]
        for mid_idx in range(row_idx):
            summed = summed - factor[row_idx][mid_idx] * forward[mid_idx]
        forward.append(summed / factor[row_idx][row_idx])
    solution = [None] * size_cols
    for row_idx in reversed(range(size_cols)):
        summed = forward[row_idx]
        for mid_idx in range(row_idx + 1, size_cols):
            summed = summed - factor[mid_idx][row_idx] * solution[mid_idx]
        solution[row_idx] = summed / factor[row_idx][row_idx]
    return jnp.stack(solution, axis=0)


def fit_statistic(values, clear, history_len, monitor_start, boundary_table):
    dates = values.shape[0]
    day = jnp.arange(dates, dtype=jnp.int32)
    design = harmonic_design(dates)
    in_history = (day < history_len[0]).astype(jnp.float32)[:, None]
    weight = clear * in_history
    outer = (design[:, :, None] * design[:, None, :]).reshape(dates, COLS * COLS)
    normal_mat = jnp.dot(
        outer.T, weight, precision=HIGH, preferred_element_type=jnp.float32
    ).reshape(COLS, COLS, -1)
    target = jnp.dot(design.T, weight * values, precision=HIGH, preferred_element_type=jnp.float32)
    coeffs = solve_batched(normal_mat, target)
    fitted = jnp.dot(design, coeffs, precision=HIGH, preferred_element_type=jnp.float32)
    resid = clear * (values - fitted)
    count = jnp.sum(weight, axis=0)
    squares = jnp.sum(weight * resid * resid, axis=0)
    sigma = jnp.sqrt(squares / (count - COLS) + 1e-06)
    lagged = day[:, None] - day[None, :]
    banded = ((lagged >= 0) & (lagged < WINDOW)).astype(jnp.float32)
    moving = jnp.dot(banded, resid, precision=HIGH, preferred_element_type=jnp.float32)
    scaled = moving / (sigma * jnp.sqrt(count))[None, :]
    bounds = boundary_table.astype(jnp.float32) * 0.001
    watching = (day >= monitor_start[0])[:, None]
    return jnp.where(watching, scaled / bounds[:, None], jnp.float32(0.0))


def per_device(values, cloud_words, history_len, monitor_start, boundary_table):
    arrived = lax.all_to_all(values, ("wide", "narrow"), split_axis=1, concat_axis=0, tiled=True)
    words = lax.all_to_all(cloud_words, ("wide", "narrow"), split_axis=1, concat_axis=0, tiled=True)
    ratio = fit_statistic(arrived, unpack_clear(words), history_len, monitor_start, boundary_table)
    rows = values.shape[0]
    blocks = ratio.reshape(ratio.shape[0] // rows, rows, ratio.shape[1])
    block_peak = lax.cummax(jnp.max(jnp.abs(blocks), axis=1), axis=0)
    earlier = jnp.concatenate([jnp.zeros_like(block_peak[:1]), block_peak[:-1]], axis=0)
    date_ratio = lax.all_to_all(ratio, ("wide", "narrow"), split_axis=0, concat_axis=1, tiled=True)
    before = lax.all_to_all(earlier, ("wide", "narrow"), split_axis=0, concat_axis=1, tiled=True)
    peak = jnp.maximum(lax.cummax(jnp.abs(date_ratio), axis=0), before)
    return (date_ratio, peak)


HISTORY_MOST = 256
MESH = pl.DeviceIdType.MESH


def host_design(dates):
    day = np.arange(dates, dtype=np.float32)
    columns = [np.ones((dates,), np.float32), (day / np.float32(dates)).astype(np.float32)]
    for harmonic in range(1, HARMONICS + 1):
        phases = (np.float32(2.0 * math.pi * harmonic / PERIOD) * day).astype(np.float64)
        columns.append(np.cos(phases).astype(np.float32))
        columns.append(np.sin(phases).astype(np.float32))
    return np.stack(columns, axis=1)


def dot_high(left, right):
    return jnp.dot(left, right, precision=HIGH, preferred_element_type=jnp.float32)


def clear_bits(words, offset, pixels):
    rows, lanes = words.shape
    parts = [((words >> (8 * k)) & 255).astype(jnp.float32).astype(jnp.bfloat16) for k in range(4)]
    stacked = jnp.concatenate(parts, axis=0)
    word_of = lax.broadcasted_iota(jnp.int32, (lanes, pixels), 1) >> 5
    spread = (lax.broadcasted_iota(jnp.int32, (lanes, pixels), 0) - offset == word_of)
    spread = spread.astype(jnp.float32).astype(jnp.bfloat16)
    wide = jnp.dot(stacked, spread, preferred_element_type=jnp.float32)
    lane = lax.broadcasted_iota(jnp.int32, (rows, pixels), 1)
    which = (lane >> 3) & 3
    byte = wide[:rows]
    for k in range(1, 4):
        byte = jnp.where(which == k, wide[k * rows : (k + 1) * rows], byte)
    return ((byte.astype(jnp.int32) >> (lane & 7)) & 1).astype(jnp.float32)


def scan_rows(array, combine, neutral):
    tiles = []
    row = lax.broadcasted_iota(jnp.int32, (8, array.shape[1]), 0)
    for at in range(0, array.shape[0], 8):
        tile = array[at : at + 8]
        for step in (1, 2, 4):
            tile = combine(tile, jnp.where(row >= step, pltpu.roll(tile, step, 0), neutral))
        if tiles:
            tile = combine(tile, tiles[-1][7:8])
        tiles.append(tile)
    return jnp.concatenate(tiles, axis=0)


def fitted(design, coeffs):
    total = design[:, 0:1] * coeffs[0:1]
    for k in range(1, COLS):
        total = total + design[:, k : k + 1] * coeffs[k : k + 1]
    return total


def solve_rows(entry, target):
    factor = [[None] * COLS for _ in range(COLS)]
    inverse = [None] * COLS
    for i in range(COLS):
        for j in range(i + 1):
            summed = entry(i, j)
            for m in range(j):
                summed = summed - factor[i][m] * factor[j][m]
            if i == j:
                inverse[i] = 1.0 / jnp.sqrt(summed)
            else:
                factor[i][j] = summed * inverse[j]
    forward = []
    for i in range(COLS):
        summed = target(i)
        for m in range(i):
            summed = summed - factor[i][m] * forward[m]
        forward.append(summed * inverse[i])
    answer = [None] * COLS
    for i in reversed(range(COLS)):
        summed = forward[i]
        for m in range(i + 1, COLS):
            summed = summed - factor[m][i] * answer[m]
        answer[i] = summed * inverse[i]
    return answer


def fused_kernel(
    narrow, chips, hist, back,
    hl_hbm, ms_hbm, b_hbm, v_hbm, w_hbm, d_hbm, ot_hbm, ratio_ref, peak_ref,
    hl_ref, ms_ref, b_ref, v_ref, w_ref, fw, cv, cw, ccl, hv, hw, ow, tp, tb, nm, cb, cnt, sq, sb, tot, tt, bf, bo, bm, sc, scb, rt, mrow, mb, dm, de, ot_ref,
    rdy_s, ax_s, ax_r, ha_s, ha_r, fw_s, fw_r, hw_s, hw_r, ow_s, ow_r, tp_s, tp_r, cb_s, cb_r, ct_s, ct_r,
    sq_s, sq_r, tt_s, tt_r, sc_s, sc_r, mx_s, mx_r, or_s, or_r, op_s, op_r, bf_s, bf_r, lc,
):
    me = lax.axis_index("wide") * narrow + lax.axis_index("narrow")
    q, c = lax.div(me, 2), lax.rem(me, 2)
    rows, pixels = v_ref.shape
    half = pixels // 2
    own = half // hist
    slots = hist
    chip_rows = 2 * rows
    late = chips - hist
    is_hist = q < hist
    is_late = q >= hist

    def dev(q2, c2):
        d = 2 * q2 + c2
        return (lax.div(d, narrow), lax.rem(d, narrow))

    def remote(src, dst, ssem, rsem, q2, c2):
        return pltpu.make_async_remote_copy(
            src_ref=src, dst_ref=dst, send_sem=ssem, recv_sem=rsem,
            device_id=dev(q2, c2), device_id_type=MESH)

    def drain(ref, sem):
        pltpu.make_async_copy(ref, ref, sem).wait()

    def cols(s):
        return pl.ds(pl.multiple_of(s * own, own), own)

    mine = pl.ds(pl.multiple_of(c * rows, rows), rows)
    theirs = pl.ds(pl.multiple_of((1 - c) * rows, rows), rows)
    my_half = pl.ds(pl.multiple_of(c * half, half), half)
    other_half = pl.ds(pl.multiple_of((1 - c) * half, half), half)

    def word_half(h):
        return pl.ds(pl.multiple_of(h * (half // 32), half // 32), half // 32)

    def half_col(h, s):
        return pl.ds(pl.multiple_of(h * half + s * own, own), own)

    get_w = pltpu.make_async_copy(w_hbm, w_ref, lc.at[6])
    get_v = pltpu.make_async_copy(v_hbm, v_ref, lc.at[7])
    keep_v = pltpu.make_async_copy(v_hbm.at[:, my_half], cv.at[mine, :], lc.at[0])
    keep_w = pltpu.make_async_copy(w_hbm, cw.at[mine, :], lc.at[1])
    get_scalars = [
        pltpu.make_async_copy(hl_hbm, hl_ref, lc.at[8]),
        pltpu.make_async_copy(ms_hbm, ms_ref, lc.at[9]),
        pltpu.make_async_copy(b_hbm, b_ref, lc.at[10]),
    ]
    barrier = pltpu.get_barrier_semaphore()
    rdy = rdy_s.at[0]

    def greet(to, sem):
        pl.semaphore_signal(
            sem, inc=1, device_id=(lax.div(to, narrow), lax.rem(to, narrow)), device_id_type=MESH)

    @pl.when(is_hist)
    def _():
        @pl.loop(1, 2 * hist)
        def _(k):
            greet(lax.rem(me + k, 2 * hist), barrier)
        greet(me + 2 * hist, barrier)

    @pl.when(is_late)
    def _():
        greet(2 * q + 1 - c, barrier)
        greet(2 * (q - back), barrier)
        greet(2 * (q - back) + 1, barrier)

    late_splits = jnp.logical_and(q >= hist + back, q < hist + 2 * back)
    late_passes = jnp.logical_and(q >= hist, q < hist + back)

    @pl.when(late_passes)
    def _():
        greet(2 * (q + back), barrier)
        greet(2 * (q + back) + 1, barrier)

    get_w.start()
    get_v.start()
    keep_w.start()
    keep_v.start()
    for get in get_scalars:
        get.start()

    swap_v = remote(v_ref.at[:, other_half], cv.at[mine, :], ax_s.at[0], ax_r.at[0], q, 1 - c)
    swap_w = remote(w_ref.at[:, word_half(1 - c)], cw.at[mine, word_half(1 - c)], ax_s.at[1], ax_r.at[1], q, 1 - c)
    came_w = remote(w_ref.at[:, word_half(c)], cw.at[theirs, word_half(c)], ax_s.at[1], ax_r.at[1], q, 1 - c)
    get_d = pltpu.make_async_copy(d_hbm.at[q], dm, lc.at[3])
    get_e = pltpu.make_async_copy(d_hbm.at[lax.max(q - back, 0)], de, lc.at[4])
    get_o = pltpu.make_async_copy(ot_hbm, ot_ref, lc.at[5])
    get_d.start()
    get_e.start()
    get_o.start()
    get_w.wait()
    get_v.wait()
    feeds = jnp.logical_and(q + back >= hist, q + back < chips)
    greeted = jnp.where(is_hist, 2 * hist - 1, 2) + jnp.where(feeds, 2, 0) + jnp.where(late_splits, 2, 0)
    pl.semaphore_wait(barrier, greeted)

    @pl.when(is_late)
    def _():
        greet(me - 2 * hist, rdy)

    swap_w.start()
    swap_v.start()

    def owner_block(q2, c2):
        return pl.ds(pl.multiple_of(lax.div(c2 * half + q2 * own, 32 * 128) * 128, 128), 128)

    my_dates = pl.ds(pl.multiple_of(me * rows, rows), rows)
    keep_o = pltpu.make_async_copy(w_ref.at[:, owner_block(q, c)], ow.at[my_dates, :], lc.at[2])

    def send_words(k):
        to = lax.rem(me + k, 2 * hist)
        return remote(w_ref.at[:, owner_block(lax.div(to, 2), lax.rem(to, 2))],
                      ow.at[my_dates, :], ow_s.at[0], ow_r.at[0],
                      lax.div(to, 2), lax.rem(to, 2))

    @pl.when(is_hist)
    def _():
        @pl.loop(1, 2 * hist)
        def _(k):
            send_words(k).start()
        keep_o.start()

    sends_early = jnp.logical_and(q + back >= hist, q + back < chips)
    splits = jnp.logical_and(q + back >= hist, is_hist)
    forwards = jnp.logical_and(q + 2 * back >= hist, q + back < hist)
    direct = slots * 3 // 8
    later = slots - 1
    middle = (direct + later) // 2

    def early_words(h):
        some = word_half(h)
        return remote(w_ref.at[:, some], hw.at[mine, some], hw_s.at[0], hw_r.at[0], q + back, h)

    def early(h, s, to):
        return remote(v_ref.at[:, half_col(h, s)], hv.at[mine, cols(s)],
                      ha_s.at[0], ha_r.at[s], to, h)

    def forward(s):
        return remote(hv.at[:, cols(s)], hv.at[:, cols(s)], fw_s.at[0], ha_r.at[s], q + 2 * back, c)

    most = slots // 2
    first = slots * 4 // 8

    def start_early(when, low, high, to):
        @pl.when(when)
        def _():
            @pl.loop(low, high)
            def _(s):
                early(0, s, to).start()
                early(1, s, to).start()

    def pass_on(low, high):
        @pl.when(forwards)
        def _():
            @pl.loop(low, high)
            def _(s):
                drain(hv.at[:, cols(s)], ha_r.at[s])
                forward(s).start()

    late_sends = jnp.logical_and(is_late, sends_early)
    late_direct = jnp.logical_and(late_sends, jnp.logical_not(late_splits))
    via = 1
    odd = lax.rem(q, 2) == 1
    odd_sends = jnp.logical_and(late_sends, odd)
    even_sends = jnp.logical_and(late_sends, jnp.logical_not(odd))

    def early_via(h, i):
        return remote(v_ref.at[:, half_col(h, most + i)], fw.at[mine, cols(i)], ha_s.at[0], fw_r.at[i], q - back, h)

    def late_forward(i):
        @pl.when(late_passes)
        def _():
            drain(fw.at[:, cols(i)], fw_r.at[i])
            remote(fw.at[:, cols(i)], hv.at[:, cols(most + i)], fw_s.at[0], ha_r.at[most + i], q + 2 * back, c).start()

    @pl.when(sends_early)
    def _():
        for h in range(2):
            early_words(h).start()

    start_early(splits, 0, direct, q + back)
    start_early(late_sends, 0, most, q + back)

    def word_block(s):
        start = c * (half // 32) + s * (own // 32)
        base = lax.div(start, 128) * 128
        return pl.ds(pl.multiple_of(base, 128), 128), start - base

    keep_w.wait()
    came_w.wait_recv()

    get_d.wait()
    get_e.wait()
    get_o.wait()
    for get in get_scalars:
        get.wait()
    keep_v.wait()
    swap_v.wait_recv()
    date = q * chip_rows + lax.broadcasted_iota(jnp.int32, (chip_rows, own), 0)

    def unpack(s):
        block, offset = word_block(s)
        ccl[:, cols(s)] = clear_bits(cw[:, block], offset, own)

    def send_target(to):
        return remote(tp.at[to], tb.at[q], tp_s.at[0], tp_r.at[0], to, c)

    columns = late // 2

    def send_coeffs(k):
        return remote(cb.at[q], cb.at[q], cb_s.at[0], cb_r.at[0], lax.rem(q + k, hist), c)

    def column_coeffs(k):
        return remote(cb.at[q - hist], cb.at[q - hist], cb_s.at[0], cb_r.at[1 + k],
                      hist + lax.rem(q - hist + 2 * k, late), c)

    def cross_coeffs(s):
        return remote(cb.at[s], cb.at[s], cb_s.at[0], cb_r.at[0], q + 1 - 2 * lax.rem(q, 2), c)

    relay = remote(cb.at[q], cb.at[q], cb_s.at[0], cb_r.at[1], q + hist, c)
    give_count = remote(cnt, cnt, ct_s.at[0], ct_r.at[0], q + hist, c)

    @pl.when(is_hist)
    def _():
        def part(s):
            unpack(s)
            weighted = jnp.where(date < hl_ref[0], ccl[:, cols(s)] * cv[:, cols(s)], 0.0)
            for k in range(COLS):
                tp[s, k : k + 1, :] = jnp.sum(weighted * dm[:, k : k + 1], axis=0, keepdims=True)

        part(lax.rem(q + 1, hist))
        part(lax.rem(q + 2, hist))
        pl.semaphore_wait(rdy, 1)
        send_target(lax.rem(q + 1, hist)).start()
        send_target(lax.rem(q + 2, hist)).start()

        @pl.loop(3, hist)
        def _(k):
            to = lax.rem(q + k, hist)
            part(to)
            send_target(to).start()

        part(q)

        start_early(splits, direct, middle, q - back)
        ratio_ref[...] = jnp.zeros_like(ratio_ref)
        peak_ref[...] = jnp.zeros_like(peak_ref)
        keep_o.wait()

        others = ow.at[pl.ds(0, (2 * hist - 1) * rows), :]
        drain(others, ow_r.at[0])

        start = c * (half // 32) + q * (own // 32)
        flags = clear_bits(ow[...], lax.rem(start, 128), own)
        day = lax.broadcasted_iota(jnp.int32, flags.shape, 0)
        nm[...] = dot_high(ot_ref[...], jnp.where(day < hl_ref[0], flags, 0.0))
        cnt[...] = nm[0:1, :]
        give_count.start()
        total = tp[q]
        drain(tb.at[pl.ds(0, hist - 1)], tp_r.at[0])

        tb[q] = total
        total = tb[0]
        for s in range(1, hist):
            total = total + tb[s]
        tb[q] = total

        def entry(i, j):
            at = i * (i + 1) // 2 + j
            return nm[at : at + 1, :]

        answer = solve_rows(entry, lambda i: tb[q, i : i + 1, :])
        for i in range(COLS):
            cb[q, i : i + 1, :] = answer[i]
        relay.start()

        @pl.loop(1, hist)
        def _(k):
            send_coeffs(k).start()

        start_early(splits, middle, later, q - back)
        start_early(splits, later, slots, q + back)
        pass_on(direct, middle)
        drain(cb.at[pl.ds(0, hist - 1)], cb_r.at[0])

    @pl.when(is_late)
    def _():
        pl.loop(0, slots)(unpack)
        drain(hw.at[:, word_half(c)], hw_r.at[0])

        @pl.loop(0, slots)
        def _(s):
            block, offset = word_block(s)
            rt[:, cols(s)] = clear_bits(hw[:, block], offset, own)

        remote(cb.at[q - hist], cb.at[q - hist], cb_s.at[0], cb_r.at[1], q - hist, c).wait_recv()

        @pl.loop(1, columns)
        def _(k):
            column_coeffs(k).start()

        cross_coeffs(q - hist).start()
        start_early(late_direct, most, most + via, q + back)
        start_early(late_sends, most + via, slots - 1, q + back)
        start_early(even_sends, slots - 1, slots, q + back)

        @pl.when(late_splits)
        def _():
            for i in range(via):
                for h in range(2):
                    early_via(h, i).start()

        @pl.loop(1, columns)
        def _(k):
            from_column = lax.rem(q - hist + late - 2 * k, late)
            drain(cb.at[from_column], cb_r.at[1 + k])
            cross_coeffs(from_column).start()

        late_forward(0)
        drain(cb.at[pl.ds(0, columns)], cb_r.at[0])

    @pl.loop(0, slots)
    def _(s):
        resid = ccl[:, cols(s)] * (cv[:, cols(s)] - fitted(dm[...], cb[s]))
        cv[:, cols(s)] = resid
        tot[0:1, cols(s)] = jnp.sum(resid, axis=0, keepdims=True)
        sq[s] = jnp.sum(jnp.where(date < hl_ref[0], resid * resid, 0.0), axis=0, keepdims=True)

    totals = jnp.logical_and(q + 1 >= hist, q + 1 < chips)
    send_total = remote(tot, tt, tt_s.at[0], tt_r.at[0], q + 1, c)

    @pl.when(totals)
    def _():
        send_total.start()

    start_early(odd_sends, slots - 1, slots, q + back)

    def send_squares(s):
        return remote(sq.at[s], sb.at[q], sq_s.at[0], sq_r.at[0], hist + s, c)

    @pl.when(is_hist)
    def _():
        @pl.loop(0, hist)
        def _(k):
            send_squares(lax.rem(q + k, hist)).start()

        pass_on(middle, later)

    def send_scale(k):
        return remote(sc, scb.at[q - hist], sc_s.at[0], sc_r.at[0],
                      hist + lax.rem(q - hist + k, late), c)

    def send_max(group, k):
        some = pl.ds(0, first) if group == 0 else pl.ds(first, slots - first)
        return remote(mrow.at[some], mb.at[q - hist, some], mx_s.at[k], mx_r.at[q - hist], hist + k, c)

    def ratio_out(s):
        return remote(rt.at[theirs, cols(s)], ratio_ref.at[:, half_col(c, s)], or_s.at[0], or_r.at[0], q, 1 - c)

    def peak_out(s):
        return remote(ccl.at[theirs, cols(s)], peak_ref.at[:, half_col(c, s)], op_s.at[0], op_r.at[0], q, 1 - c)

    give_before = remote(bf, bo, bf_s.at[0], bf_r.at[0], q, 1 - c)

    @pl.when(is_late)
    def _():
        row = lax.broadcasted_iota(jnp.int32, (chip_rows, 128), 0)
        bounds = jnp.zeros((chip_rows, 128), jnp.int32)
        for i in range(chip_rows):
            bounds = jnp.where(row == i, b_ref[q * chip_rows + i], bounds)
        over = 1.0 / (bounds[:, 0:1].astype(jnp.float32) * 0.001)

        def window(s):
            drain(hv.at[:, cols(s)], ha_r.at[s])
            early_resid = rt[:, cols(s)] * (hv[:, cols(s)] - fitted(de[...], cb[s]))
            change = cv[:, cols(s)] - early_resid
            return scan_rows(change, jnp.add, 0.0) + jnp.sum(early_resid, axis=0, keepdims=True)

        def statistic(s, partial):
            moving = partial + tt[0:1, cols(s)]
            ratio = jnp.where(date >= ms_ref[0], moving * over, 0.0)
            rt[:, cols(s)] = ratio
            best = scan_rows(jnp.abs(ratio), jnp.maximum, 0.0)
            ccl[:, cols(s)] = best
            mrow[s] = best[chip_rows - 1 :, :]

        def send_maxima(group):
            @pl.loop(q - hist + 1, late)
            def _(k):
                send_max(group, k).start()

        @pl.loop(0, first)
        def _(s):
            rt[:, cols(s)] = window(s)

        drain(sb, sq_r.at[0])
        give_count.wait_recv()
        squares = sb[0]
        for s in range(1, hist):
            squares = squares + sb[s]
        count = cnt[...]
        sigma = jnp.sqrt(squares / (count - COLS) + 1e-06)
        scale = 1.0 / (sigma * jnp.sqrt(count))
        sc[...] = scale
        scb[q - hist] = scale

        @pl.loop(1, late)
        def _(k):
            send_scale(k).start()

        send_total.wait_recv()

        @pl.loop(0, first)
        def _(s):
            statistic(s, rt[:, cols(s)])

        send_maxima(0)

        @pl.loop(first, slots)
        def _(s):
            statistic(s, window(s))

        send_maxima(1)
        drain(scb.at[pl.ds(0, late - 1)], sc_r.at[0])

        @pl.loop(0, slots)
        def _(s):
            scaled = rt[:, cols(s)] * scb[s]
            rt[:, cols(s)] = scaled
            ratio_out(s).start()
            ratio_ref[:, half_col(c, s)] = rt[mine, cols(s)]
            ccl[:, cols(s)] = ccl[:, cols(s)] * scb[s]
            peak_out(s).start()

        bm[...] = jnp.zeros_like(bm)

        @pl.loop(0, q - hist)
        def _(k):
            drain(mrow, mx_r.at[k])
            bm[...] = jnp.maximum(bm[...], mb[k])

        for s in range(slots):
            bf[0:1, s * own : (s + 1) * own] = bm[s] * scb[s]

        give_before.start()

        @pl.loop(0, slots)
        def _(s):
            peak_ref[:, half_col(c, s)] = jnp.maximum(ccl[mine, cols(s)], bf[0:1, cols(s)])

        drain(ratio_ref.at[:, other_half], or_r.at[0])
        drain(peak_ref.at[:, other_half], op_r.at[0])
        give_before.wait_recv()

        @pl.loop(0, slots)
        def _(s):
            other = half_col(1 - c, s)
            peak_ref[:, other] = jnp.maximum(peak_ref[:, other], bo[0:1, cols(s)])

        give_before.wait_send()
        drain(ratio_ref.at[:, other_half], or_s.at[0])
        drain(peak_ref.at[:, other_half], op_s.at[0])

        @pl.loop(q - hist + 1, late)
        def _(k):
            drain(mrow, mx_s.at[k])

        drain(scb.at[pl.ds(0, late - 1)], sc_s.at[0])
        drain(cb.at[pl.ds(0, hist - 1)], cb_s.at[0])

    swap_v.wait_send()
    swap_w.wait_send()

    @pl.when(is_hist)
    def _():
        drain(ow.at[pl.ds(0, (2 * hist - 1) * rows), :], ow_s.at[0])
        drain(tb.at[pl.ds(0, hist - 1)], tp_s.at[0])
        drain(cb, cb_s.at[0])
        give_count.wait_send()
        drain(sq, sq_s.at[0])

    @pl.when(totals)
    def _():
        send_total.wait_send()

    @pl.when(sends_early)
    def _():
        drain(w_ref, hw_s.at[0])
        drain(v_ref, ha_s.at[0])

    @pl.when(late_passes)
    def _():
        drain(fw, fw_s.at[0])

    @pl.when(forwards)
    def _():
        drain(hv.at[:, pl.ds(direct * own, (later - direct) * own)], fw_s.at[0])


def store_kernel(ratio_ref, peak_ref, ratio_hbm, peak_hbm, sems):
    copies = [
        pltpu.make_async_copy(ratio_ref, ratio_hbm, sems.at[0]),
        pltpu.make_async_copy(peak_ref, peak_hbm, sems.at[1]),
    ]
    for copy in copies:
        copy.start()
    for copy in copies:
        copy.wait()


def fused_device(narrow, devices, values, cloud_words, history_len, monitor_start, boundary_table):
    rows, pixels = values.shape
    chips, chip_rows, half = devices // 2, 2 * rows, pixels // 2
    dates = boundary_table.shape[0]
    hist, back = HISTORY_MOST // chip_rows, WINDOW // chip_rows
    own, late = half // hist, chips - hist
    design = host_design(dates)
    lower = [(i, j) for i in range(COLS) for j in range(i + 1)]
    outer = np.zeros((40, HISTORY_MOST), np.float32)
    for at, (i, j) in enumerate(lower):
        outer[at] = design[:HISTORY_MOST, i] * design[:HISTORY_MOST, j]
    by_chip = design.reshape(chips, chip_rows, COLS)
    hbm = pl.BlockSpec(memory_space=pltpu.HBM)
    f32, i32, dma = jnp.float32, jnp.int32, pltpu.SemaphoreType.DMA
    scratch = [
        pltpu.SMEM((1,), i32),
        pltpu.SMEM((1,), i32),
        pltpu.SMEM((dates,), i32),
        pltpu.VMEM((rows, pixels), f32),
        pltpu.VMEM((rows, pixels // 32), i32),
        pltpu.VMEM((chip_rows, own), f32),
        pltpu.VMEM((chip_rows, half), f32),
        pltpu.VMEM((chip_rows, pixels // 32), i32),
        pltpu.VMEM((chip_rows, half), f32),
        pltpu.VMEM((chip_rows, half), f32),
        pltpu.VMEM((chip_rows, pixels // 32), i32),
        pltpu.VMEM((HISTORY_MOST, 128), i32),
        pltpu.VMEM((hist, COLS, own), f32),
        pltpu.VMEM((hist, COLS, own), f32),
        pltpu.VMEM((40, own), f32),
        pltpu.VMEM((hist, COLS, own), f32),
        pltpu.VMEM((1, own), f32),
        pltpu.VMEM((hist, 1, own), f32),
        pltpu.VMEM((hist, 1, own), f32),
        pltpu.VMEM((1, half), f32),
        pltpu.VMEM((1, half), f32),
        pltpu.VMEM((1, half), f32),
        pltpu.VMEM((1, half), f32),
        pltpu.VMEM((hist, 1, own), f32),
        pltpu.VMEM((1, own), f32),
        pltpu.VMEM((late, 1, own), f32),
        pltpu.VMEM((chip_rows, half), f32),
        pltpu.VMEM((hist, 1, own), f32),
        pltpu.VMEM((late, hist, 1, own), f32),
        pltpu.VMEM((chip_rows, COLS), f32),
        pltpu.VMEM((chip_rows, COLS), f32),
        pltpu.VMEM((40, HISTORY_MOST), f32),
    ]
    scratch += [pltpu.SemaphoreType.REGULAR((1,))]
    scratch += [dma((2,)), dma((2,)), dma((1,)), dma((hist,)), dma((1,)), dma((1,))]
    for number in (1, 1, 1):
        scratch += [dma((number,)), dma((number,))]
    scratch += [dma((1,)), dma((1 + late // 2,))]
    for number in (1, 1):
        scratch += [dma((number,)), dma((number,))]
    scratch += [dma((1,)), dma((1,))]
    for number in (1, late, 1, 1, 1):
        scratch += [dma((number,)), dma((number,))]
    scratch.append(dma((11,)))
    outs = pl.pallas_call(
        functools.partial(fused_kernel, narrow, chips, hist, back),
        out_shape=[pltpu.VMEM((rows, pixels), f32)] * 2,
        in_specs=[hbm] * 7,
        scratch_shapes=scratch,
        compiler_params=pltpu.CompilerParams(
            has_side_effects=True, collective_id=0, vmem_limit_bytes=67043328 - 2 * rows * pixels * 4),
    )(
        history_len, monitor_start, boundary_table, values, cloud_words,
        jnp.asarray(by_chip), jnp.asarray(outer),
    )
    return pl.pallas_call(
        store_kernel,
        out_shape=[jax.ShapeDtypeStruct((rows, pixels), f32)] * 2,
        in_specs=[pl.BlockSpec(memory_space=pltpu.VMEM)] * 2,
        out_specs=[pl.BlockSpec(memory_space=pl.ANY)] * 2,
        scratch_shapes=[dma((2,))],
        compiler_params=pltpu.CompilerParams(vmem_limit_bytes=8 * 1024 * 1024),
    )(*outs)


def fits(narrow, devices, rows, pixels):
    chip_rows = 2 * rows
    if narrow % 2 or rows % 8 or HISTORY_MOST % chip_rows or WINDOW != 2 * chip_rows:
        return False
    hist = HISTORY_MOST // chip_rows
    return devices // 2 == 2 * hist and (pixels // 2) % (hist * 128) == 0 and 128 % (pixels // 64 // hist) == 0


def solution(mesh):
    narrow = mesh.shape["narrow"]
    devices = narrow * mesh.shape["wide"]

    def per_device_any(values, *rest):
        if fits(narrow, devices, *values.shape):
            return fused_device(narrow, devices, values, *rest)
        return per_device(values, *rest)

    placed = (P(("wide", "narrow"), None), P(("wide", "narrow"), None), P(), P(), P())
    return jax.shard_map(
        per_device_any,
        mesh=mesh,
        in_specs=placed,
        out_specs=(P(("wide", "narrow"), None), P(("wide", "narrow"), None)),
        check_vma=False,
    )
```

```python
import functools
import math

import jax
import jax.numpy as jnp
from jax import lax
from jax.experimental import pallas as pl
from jax.experimental.pallas import tpu as pltpu
import numpy as np
from jax.sharding import PartitionSpec as P

PERIOD = 46
HARMONICS = 3
COLS = 8
WINDOW = 64


HIGH = lax.Precision.HIGHEST


def unpack_clear(words):
    shifts = jnp.arange(32, dtype=jnp.int32)
    flags = jnp.bitwise_and(jnp.right_shift(words[:, :, None], shifts[None, None, :]), jnp.int32(1))
    return flags.reshape(words.shape[0], words.shape[1] * 32).astype(jnp.float32)


def harmonic_design(dates):
    day_float = jnp.arange(dates, dtype=jnp.int32).astype(jnp.float32)
    columns = [jnp.ones((dates,), jnp.float32), day_float / dates]
    for harmonic in range(1, HARMONICS + 1):
        phases = 2.0 * math.pi * harmonic / PERIOD * day_float
        columns.append(jnp.cos(phases))
        columns.append(jnp.sin(phases))
    return jnp.stack(columns, axis=1)


def solve_batched(normal_mat, target):
    size_cols = normal_mat.shape[0]
    factor = [[None] * size_cols for row_idx in range(size_cols)]
    for row_idx in range(size_cols):
        for col_idx in range(row_idx + 1):
            summed = normal_mat[row_idx, col_idx]
            for mid_idx in range(col_idx):
                summed = summed - factor[row_idx][mid_idx] * factor[col_idx][mid_idx]
            if row_idx == col_idx:
                factor[row_idx][col_idx] = jnp.sqrt(summed)
            else:
                factor[row_idx][col_idx] = summed / factor[col_idx][col_idx]
    forward = []
    for row_idx in range(size_cols):
        summed = target[row_idx]
        for mid_idx in range(row_idx):
            summed = summed - factor[row_idx][mid_idx] * forward[mid_idx]
        forward.append(summed / factor[row_idx][row_idx])
    solution = [None] * size_cols
    for row_idx in reversed(range(size_cols)):
        summed = forward[row_idx]
        for mid_idx in range(row_idx + 1, size_cols):
            summed = summed - factor[mid_idx][row_idx] * solution[mid_idx]
        solution[row_idx] = summed / factor[row_idx][row_idx]
    return jnp.stack(solution, axis=0)


def fit_statistic(values, clear, history_len, monitor_start, boundary_table):
    dates = values.shape[0]
    day = jnp.arange(dates, dtype=jnp.int32)
    design = harmonic_design(dates)
    in_history = (day < history_len[0]).astype(jnp.float32)[:, None]
    weight = clear * in_history
    outer = (design[:, :, None] * design[:, None, :]).reshape(dates, COLS * COLS)
    normal_mat = jnp.dot(
        outer.T, weight, precision=HIGH, preferred_element_type=jnp.float32
    ).reshape(COLS, COLS, -1)
    target = jnp.dot(design.T, weight * values, precision=HIGH, preferred_element_type=jnp.float32)
    coeffs = solve_batched(normal_mat, target)
    fitted = jnp.dot(design, coeffs, precision=HIGH, preferred_element_type=jnp.float32)
    resid = clear * (values - fitted)
    count = jnp.sum(weight, axis=0)
    squares = jnp.sum(weight * resid * resid, axis=0)
    sigma = jnp.sqrt(squares / (count - COLS) + 1e-06)
    lagged = day[:, None] - day[None, :]
    banded = ((lagged >= 0) & (lagged < WINDOW)).astype(jnp.float32)
    moving = jnp.dot(banded, resid, precision=HIGH, preferred_element_type=jnp.float32)
    scaled = moving / (sigma * jnp.sqrt(count))[None, :]
    bounds = boundary_table.astype(jnp.float32) * 0.001
    watching = (day >= monitor_start[0])[:, None]
    return jnp.where(watching, scaled / bounds[:, None], jnp.float32(0.0))


def per_device(values, cloud_words, history_len, monitor_start, boundary_table):
    arrived = lax.all_to_all(values, ("wide", "narrow"), split_axis=1, concat_axis=0, tiled=True)
    words = lax.all_to_all(cloud_words, ("wide", "narrow"), split_axis=1, concat_axis=0, tiled=True)
    ratio = fit_statistic(arrived, unpack_clear(words), history_len, monitor_start, boundary_table)
    rows = values.shape[0]
    blocks = ratio.reshape(ratio.shape[0] // rows, rows, ratio.shape[1])
    block_peak = lax.cummax(jnp.max(jnp.abs(blocks), axis=1), axis=0)
    earlier = jnp.concatenate([jnp.zeros_like(block_peak[:1]), block_peak[:-1]], axis=0)
    date_ratio = lax.all_to_all(ratio, ("wide", "narrow"), split_axis=0, concat_axis=1, tiled=True)
    before = lax.all_to_all(earlier, ("wide", "narrow"), split_axis=0, concat_axis=1, tiled=True)
    peak = jnp.maximum(lax.cummax(jnp.abs(date_ratio), axis=0), before)
    return (date_ratio, peak)


HISTORY_MOST = 256
MESH = pl.DeviceIdType.MESH


def host_design(dates):
    day = np.arange(dates, dtype=np.float32)
    columns = [np.ones((dates,), np.float32), (day / np.float32(dates)).astype(np.float32)]
    for harmonic in range(1, HARMONICS + 1):
        phases = (np.float32(2.0 * math.pi * harmonic / PERIOD) * day).astype(np.float64)
        columns.append(np.cos(phases).astype(np.float32))
        columns.append(np.sin(phases).astype(np.float32))
    return np.stack(columns, axis=1)


def dot_high(left, right):
    return jnp.dot(left, right, precision=HIGH, preferred_element_type=jnp.float32)


def clear_bits(words, offset, pixels):
    rows, lanes = words.shape
    parts = [((words >> (8 * k)) & 255).astype(jnp.float32).astype(jnp.bfloat16) for k in range(4)]
    stacked = jnp.concatenate(parts, axis=0)
    word_of = lax.broadcasted_iota(jnp.int32, (lanes, pixels), 1) >> 5
    spread = (lax.broadcasted_iota(jnp.int32, (lanes, pixels), 0) - offset == word_of)
    spread = spread.astype(jnp.float32).astype(jnp.bfloat16)
    wide = jnp.dot(stacked, spread, preferred_element_type=jnp.float32)
    lane = lax.broadcasted_iota(jnp.int32, (rows, pixels), 1)
    which = (lane >> 3) & 3
    byte = wide[:rows]
    for k in range(1, 4):
        byte = jnp.where(which == k, wide[k * rows : (k + 1) * rows], byte)
    return ((byte.astype(jnp.int32) >> (lane & 7)) & 1).astype(jnp.float32)


def scan_rows(array, combine, neutral):
    tiles = []
    row = lax.broadcasted_iota(jnp.int32, (8, array.shape[1]), 0)
    for at in range(0, array.shape[0], 8):
        tile = array[at : at + 8]
        for step in (1, 2, 4):
            tile = combine(tile, jnp.where(row >= step, pltpu.roll(tile, step, 0), neutral))
        if tiles:
            tile = combine(tile, tiles[-1][7:8])
        tiles.append(tile)
    return jnp.concatenate(tiles, axis=0)


def fitted(design, coeffs):
    total = design[:, 0:1] * coeffs[0:1]
    for k in range(1, COLS):
        total = total + design[:, k : k + 1] * coeffs[k : k + 1]
    return total


def solve_rows(entry, target):
    factor = [[None] * COLS for _ in range(COLS)]
    inverse = [None] * COLS
    for i in range(COLS):
        for j in range(i + 1):
            summed = entry(i, j)
            for m in range(j):
                summed = summed - factor[i][m] * factor[j][m]
            if i == j:
                inverse[i] = 1.0 / jnp.sqrt(summed)
            else:
                factor[i][j] = summed * inverse[j]
    forward = []
    for i in range(COLS):
        summed = target(i)
        for m in range(i):
            summed = summed - factor[i][m] * forward[m]
        forward.append(summed * inverse[i])
    answer = [None] * COLS
    for i in reversed(range(COLS)):
        summed = forward[i]
        for m in range(i + 1, COLS):
            summed = summed - factor[m][i] * answer[m]
        answer[i] = summed * inverse[i]
    return answer


def fused_kernel(
    narrow, chips, hist, back,
    hl_hbm, ms_hbm, b_hbm, v_hbm, w_hbm, d_hbm, ot_hbm, ratio_ref, peak_ref,
    hl_ref, ms_ref, b_ref, v_ref, w_ref, fw, cv, cw, ccl, hv, hw, ow, tp, tb, nm, cb, cnt, sq, sb, tot, tt, bf, bo, bm, sc, scb, rt, mrow, mb, dm, de, ot_ref,
    rdy_s, ax_s, ax_r, ha_s, ha_r, fw_s, fw_r, hw_s, hw_r, ow_s, ow_r, tp_s, tp_r, cb_s, cb_r, ct_s, ct_r,
    sq_s, sq_r, tt_s, tt_r, sc_s, sc_r, mx_s, mx_r, or_s, or_r, op_s, op_r, bf_s, bf_r, lc,
):
    me = lax.axis_index("wide") * narrow + lax.axis_index("narrow")
    q, c = lax.div(me, 2), lax.rem(me, 2)
    rows, pixels = v_ref.shape
    half = pixels // 2
    own = half // hist
    slots = hist
    chip_rows = 2 * rows
    late = chips - hist
    is_hist = q < hist
    is_late = q >= hist

    def dev(q2, c2):
        d = 2 * q2 + c2
        return (lax.div(d, narrow), lax.rem(d, narrow))

    def remote(src, dst, ssem, rsem, q2, c2):
        return pltpu.make_async_remote_copy(
            src_ref=src, dst_ref=dst, send_sem=ssem, recv_sem=rsem,
            device_id=dev(q2, c2), device_id_type=MESH)

    def drain(ref, sem):
        pltpu.make_async_copy(ref, ref, sem).wait()

    def cols(s):
        return pl.ds(pl.multiple_of(s * own, own), own)

    mine = pl.ds(pl.multiple_of(c * rows, rows), rows)
    theirs = pl.ds(pl.multiple_of((1 - c) * rows, rows), rows)
    my_half = pl.ds(pl.multiple_of(c * half, half), half)
    other_half = pl.ds(pl.multiple_of((1 - c) * half, half), half)

    def word_half(h):
        return pl.ds(pl.multiple_of(h * (half // 32), half // 32), half // 32)

    def half_col(h, s):
        return pl.ds(pl.multiple_of(h * half + s * own, own), own)

    get_w = pltpu.make_async_copy(w_hbm, w_ref, lc.at[6])
    get_v = pltpu.make_async_copy(v_hbm, v_ref, lc.at[7])
    keep_v = pltpu.make_async_copy(v_hbm.at[:, my_half], cv.at[mine, :], lc.at[0])
    keep_w = pltpu.make_async_copy(w_hbm, cw.at[mine, :], lc.at[1])
    get_scalars = [
        pltpu.make_async_copy(hl_hbm, hl_ref, lc.at[8]),
        pltpu.make_async_copy(ms_hbm, ms_ref, lc.at[9]),
        pltpu.make_async_copy(b_hbm, b_ref, lc.at[10]),
    ]
    barrier = pltpu.get_barrier_semaphore()
    rdy = rdy_s.at[0]

    def greet(to, sem):
        pl.semaphore_signal(
            sem, inc=1, device_id=(lax.div(to, narrow), lax.rem(to, narrow)), device_id_type=MESH)

    @pl.when(is_hist)
    def _():
        @pl.loop(1, 2 * hist)
        def _(k):
            greet(lax.rem(me + k, 2 * hist), barrier)
        greet(me + 2 * hist, barrier)

    @pl.when(is_late)
    def _():
        greet(2 * q + 1 - c, barrier)
        greet(2 * (q - back), barrier)
        greet(2 * (q - back) + 1, barrier)

    late_splits = jnp.logical_and(q >= hist + back, q < hist + 2 * back)
    late_passes = jnp.logical_and(q >= hist, q < hist + back)

    @pl.when(late_passes)
    def _():
        greet(2 * (q + back), barrier)
        greet(2 * (q + back) + 1, barrier)

    get_w.start()
    get_v.start()
    keep_w.start()
    keep_v.start()
    for get in get_scalars:
        get.start()

    swap_v = remote(v_ref.at[:, other_half], cv.at[mine, :], ax_s.at[0], ax_r.at[0], q, 1 - c)
    swap_w = remote(w_ref.at[:, word_half(1 - c)], cw.at[mine, word_half(1 - c)], ax_s.at[1], ax_r.at[1], q, 1 - c)
    came_w = remote(w_ref.at[:, word_half(c)], cw.at[theirs, word_half(c)], ax_s.at[1], ax_r.at[1], q, 1 - c)
    get_d = pltpu.make_async_copy(d_hbm.at[q], dm, lc.at[3])
    get_e = pltpu.make_async_copy(d_hbm.at[lax.max(q - back, 0)], de, lc.at[4])
    get_o = pltpu.make_async_copy(ot_hbm, ot_ref, lc.at[5])
    get_d.start()
    get_e.start()
    get_o.start()
    get_w.wait()
    get_v.wait()
    feeds = jnp.logical_and(q + back >= hist, q + back < chips)
    greeted = jnp.where(is_hist, 2 * hist - 1, 2) + jnp.where(feeds, 2, 0) + jnp.where(late_splits, 2, 0)
    pl.semaphore_wait(barrier, greeted)

    @pl.when(is_late)
    def _():
        greet(me - 2 * hist, rdy)

    swap_w.start()
    swap_v.start()

    def owner_block(q2, c2):
        return pl.ds(pl.multiple_of(lax.div(c2 * half + q2 * own, 32 * 128) * 128, 128), 128)

    my_dates = pl.ds(pl.multiple_of(me * rows, rows), rows)
    keep_o = pltpu.make_async_copy(w_ref.at[:, owner_block(q, c)], ow.at[my_dates, :], lc.at[2])

    def send_words(k):
        to = lax.rem(me + k, 2 * hist)
        return remote(w_ref.at[:, owner_block(lax.div(to, 2), lax.rem(to, 2))],
                      ow.at[my_dates, :], ow_s.at[0], ow_r.at[0],
                      lax.div(to, 2), lax.rem(to, 2))

    @pl.when(is_hist)
    def _():
        @pl.loop(1, 2 * hist)
        def _(k):
            send_words(k).start()
        keep_o.start()

    sends_early = jnp.logical_and(q + back >= hist, q + back < chips)
    splits = jnp.logical_and(q + back >= hist, is_hist)
    forwards = jnp.logical_and(q + 2 * back >= hist, q + back < hist)
    direct = slots * 3 // 8
    later = slots - 1
    middle = (direct + later) // 2

    def early_words(h):
        some = word_half(h)
        return remote(w_ref.at[:, some], hw.at[mine, some], hw_s.at[0], hw_r.at[0], q + back, h)

    def early(h, s, to):
        return remote(v_ref.at[:, half_col(h, s)], hv.at[mine, cols(s)],
                      ha_s.at[0], ha_r.at[s], to, h)

    def forward(s):
        return remote(hv.at[:, cols(s)], hv.at[:, cols(s)], fw_s.at[0], ha_r.at[s], q + 2 * back, c)

    most = slots // 2
    first = slots * 4 // 8
    ready = slots * 6 // 8

    def start_early(when, low, high, to):
        @pl.when(when)
        def _():
            @pl.loop(low, high)
            def _(s):
                early(0, s, to).start()
                early(1, s, to).start()

    def pass_on(low, high):
        @pl.when(forwards)
        def _():
            @pl.loop(low, high)
            def _(s):
                drain(hv.at[:, cols(s)], ha_r.at[s])
                forward(s).start()

    late_sends = jnp.logical_and(is_late, sends_early)
    late_direct = jnp.logical_and(late_sends, jnp.logical_not(late_splits))
    via = 1
    odd = jnp.logical_and(lax.rem(q, 2) == 1, q + back + 1 < chips)
    odd_sends = jnp.logical_and(late_sends, odd)
    even_sends = jnp.logical_and(late_sends, jnp.logical_not(odd))

    def early_via(h, i):
        return remote(v_ref.at[:, half_col(h, most + i)], fw.at[mine, cols(i)], ha_s.at[0], fw_r.at[i], q - back, h)

    def late_forward(i):
        @pl.when(late_passes)
        def _():
            drain(fw.at[:, cols(i)], fw_r.at[i])
            remote(fw.at[:, cols(i)], hv.at[:, cols(most + i)], fw_s.at[0], ha_r.at[most + i], q + 2 * back, c).start()

    @pl.when(sends_early)
    def _():
        for h in range(2):
            early_words(h).start()

    start_early(splits, 0, direct, q + back)
    start_early(late_sends, 0, most, q + back)

    def word_block(s):
        start = c * (half // 32) + s * (own // 32)
        base = lax.div(start, 128) * 128
        return pl.ds(pl.multiple_of(base, 128), 128), start - base

    keep_w.wait()
    came_w.wait_recv()

    get_d.wait()
    get_e.wait()
    get_o.wait()
    for get in get_scalars:
        get.wait()
    keep_v.wait()
    swap_v.wait_recv()
    date = q * chip_rows + lax.broadcasted_iota(jnp.int32, (chip_rows, own), 0)

    def unpack(s):
        block, offset = word_block(s)
        ccl[:, cols(s)] = clear_bits(cw[:, block], offset, own)

    def send_target(to):
        return remote(tp.at[to], tb.at[q], tp_s.at[0], tp_r.at[0], to, c)

    columns = late // 2

    def send_coeffs(k):
        return remote(cb.at[q], cb.at[q], cb_s.at[0], cb_r.at[0], lax.rem(q + k, hist), c)

    def column_coeffs(k):
        return remote(cb.at[q - hist], cb.at[q - hist], cb_s.at[0], cb_r.at[1 + k],
                      hist + lax.rem(q - hist + 2 * k, late), c)

    def cross_coeffs(s):
        return remote(cb.at[s], cb.at[s], cb_s.at[0], cb_r.at[0], q + 1 - 2 * lax.rem(q, 2), c)

    relay = remote(cb.at[q], cb.at[q], cb_s.at[0], cb_r.at[1], q + hist, c)
    give_count = remote(cnt, cnt, ct_s.at[0], ct_r.at[0], q + hist, c)

    @pl.when(is_hist)
    def _():
        def part(s):
            unpack(s)
            weighted = jnp.where(date < hl_ref[0], ccl[:, cols(s)] * cv[:, cols(s)], 0.0)
            for k in range(COLS):
                tp[s, k : k + 1, :] = jnp.sum(weighted * dm[:, k : k + 1], axis=0, keepdims=True)

        part(lax.rem(q + 1, hist))
        part(lax.rem(q + 2, hist))
        pl.semaphore_wait(rdy, 1)
        send_target(lax.rem(q + 1, hist)).start()
        send_target(lax.rem(q + 2, hist)).start()

        @pl.loop(3, hist)
        def _(k):
            to = lax.rem(q + k, hist)
            part(to)
            send_target(to).start()

        part(q)

        start_early(splits, direct, middle, q - back)
        ratio_ref[...] = jnp.zeros_like(ratio_ref)
        peak_ref[...] = jnp.zeros_like(peak_ref)
        keep_o.wait()

        others = ow.at[pl.ds(0, (2 * hist - 1) * rows), :]
        drain(others, ow_r.at[0])

        start = c * (half // 32) + q * (own // 32)
        flags = clear_bits(ow[...], lax.rem(start, 128), own)
        day = lax.broadcasted_iota(jnp.int32, flags.shape, 0)
        nm[...] = dot_high(ot_ref[...], jnp.where(day < hl_ref[0], flags, 0.0))
        cnt[...] = nm[0:1, :]
        give_count.start()
        total = tp[q]
        drain(tb.at[pl.ds(0, hist - 1)], tp_r.at[0])

        tb[q] = total
        total = tb[0]
        for s in range(1, hist):
            total = total + tb[s]
        tb[q] = total

        def entry(i, j):
            at = i * (i + 1) // 2 + j
            return nm[at : at + 1, :]

        answer = solve_rows(entry, lambda i: tb[q, i : i + 1, :])
        for i in range(COLS):
            cb[q, i : i + 1, :] = answer[i]
        relay.start()

        @pl.loop(1, hist)
        def _(k):
            send_coeffs(k).start()

        start_early(splits, middle, later, q - back)
        start_early(splits, later, slots, q + back)
        pass_on(direct, middle)
        drain(cb.at[pl.ds(0, hist - 1)], cb_r.at[0])

    @pl.when(is_late)
    def _():
        pl.loop(0, slots)(unpack)
        drain(hw.at[:, word_half(c)], hw_r.at[0])

        @pl.loop(0, slots)
        def _(s):
            block, offset = word_block(s)
            rt[:, cols(s)] = clear_bits(hw[:, block], offset, own)

        remote(cb.at[q - hist], cb.at[q - hist], cb_s.at[0], cb_r.at[1], q - hist, c).wait_recv()

        @pl.loop(1, columns)
        def _(k):
            column_coeffs(k).start()

        cross_coeffs(q - hist).start()
        start_early(late_direct, most, most + via, q + back)
        start_early(late_sends, most + via, slots - 1, q + back)
        start_early(even_sends, slots - 1, slots, q + back)

        @pl.when(late_splits)
        def _():
            for i in range(via):
                for h in range(2):
                    early_via(h, i).start()

        @pl.loop(1, columns)
        def _(k):
            from_column = lax.rem(q - hist + late - 2 * k, late)
            drain(cb.at[from_column], cb_r.at[1 + k])
            cross_coeffs(from_column).start()

        late_forward(0)
        drain(cb.at[pl.ds(0, columns)], cb_r.at[0])

    @pl.loop(0, slots)
    def _(s):
        resid = ccl[:, cols(s)] * (cv[:, cols(s)] - fitted(dm[...], cb[s]))
        cv[:, cols(s)] = resid
        tot[0:1, cols(s)] = jnp.sum(resid, axis=0, keepdims=True)
        sq[s] = jnp.sum(jnp.where(date < hl_ref[0], resid * resid, 0.0), axis=0, keepdims=True)

    totals = jnp.logical_and(q + 1 >= hist, q + 1 < chips)
    send_total = remote(tot, tt, tt_s.at[0], tt_r.at[0], q + 1, c)

    @pl.when(totals)
    def _():
        send_total.start()

    start_early(odd_sends, slots - 1, slots, q + back)

    def send_squares(s):
        return remote(sq.at[s], sb.at[q], sq_s.at[0], sq_r.at[0], hist + s, c)

    @pl.when(is_hist)
    def _():
        @pl.loop(0, hist)
        def _(k):
            send_squares(lax.rem(q + k, hist)).start()

        pass_on(middle, later)

    def send_scale(k):
        return remote(sc, scb.at[q - hist], sc_s.at[0], sc_r.at[0],
                      hist + lax.rem(q - hist + k, late), c)

    def send_max(group, k):
        some = pl.ds(0, first) if group == 0 else pl.ds(first, slots - first)
        return remote(mrow.at[some], mb.at[q - hist, some], mx_s.at[k], mx_r.at[q - hist], hist + k, c)

    def ratio_out(s):
        return remote(rt.at[theirs, cols(s)], ratio_ref.at[:, half_col(c, s)], or_s.at[0], or_r.at[0], q, 1 - c)

    def peak_out(s):
        return remote(ccl.at[theirs, cols(s)], peak_ref.at[:, half_col(c, s)], op_s.at[0], op_r.at[0], q, 1 - c)

    give_before = remote(bf, bo, bf_s.at[0], bf_r.at[0], q, 1 - c)

    @pl.when(is_late)
    def _():
        row = lax.broadcasted_iota(jnp.int32, (chip_rows, 128), 0)
        bounds = jnp.zeros((chip_rows, 128), jnp.int32)
        for i in range(chip_rows):
            bounds = jnp.where(row == i, b_ref[q * chip_rows + i], bounds)
        over = 1.0 / (bounds[:, 0:1].astype(jnp.float32) * 0.001)

        def window(s):
            drain(hv.at[:, cols(s)], ha_r.at[s])
            early_resid = rt[:, cols(s)] * (hv[:, cols(s)] - fitted(de[...], cb[s]))
            change = cv[:, cols(s)] - early_resid
            return scan_rows(change, jnp.add, 0.0) + jnp.sum(early_resid, axis=0, keepdims=True)

        def statistic(s, partial):
            moving = partial + tt[0:1, cols(s)]
            ratio = jnp.where(date >= ms_ref[0], moving * over, 0.0)
            rt[:, cols(s)] = ratio
            best = scan_rows(jnp.abs(ratio), jnp.maximum, 0.0)
            ccl[:, cols(s)] = best
            mrow[s] = best[chip_rows - 1 :, :]

        def send_maxima(group):
            @pl.loop(q - hist + 1, late)
            def _(k):
                send_max(group, k).start()

        @pl.loop(0, first)
        def _(s):
            rt[:, cols(s)] = window(s)

        drain(sb, sq_r.at[0])
        give_count.wait_recv()
        squares = sb[0]
        for s in range(1, hist):
            squares = squares + sb[s]
        count = cnt[...]
        sigma = jnp.sqrt(squares / (count - COLS) + 1e-06)
        scale = 1.0 / (sigma * jnp.sqrt(count))
        sc[...] = scale
        scb[q - hist] = scale

        @pl.loop(1, late)
        def _(k):
            send_scale(k).start()

        @pl.loop(first, ready)
        def _(s):
            rt[:, cols(s)] = window(s)

        send_total.wait_recv()

        @pl.loop(0, first)
        def _(s):
            statistic(s, rt[:, cols(s)])

        send_maxima(0)

        @pl.loop(first, ready)
        def _(s):
            statistic(s, rt[:, cols(s)])

        @pl.loop(ready, slots)
        def _(s):
            statistic(s, window(s))

        send_maxima(1)
        drain(scb.at[pl.ds(0, late - 1)], sc_r.at[0])

        @pl.loop(0, slots)
        def _(s):
            scaled = rt[:, cols(s)] * scb[s]
            rt[:, cols(s)] = scaled
            ratio_out(s).start()
            ratio_ref[:, half_col(c, s)] = rt[mine, cols(s)]
            ccl[:, cols(s)] = ccl[:, cols(s)] * scb[s]
            peak_out(s).start()

        bm[...] = jnp.zeros_like(bm)

        @pl.loop(0, q - hist)
        def _(k):
            drain(mrow, mx_r.at[k])
            bm[...] = jnp.maximum(bm[...], mb[k])

        for s in range(slots):
            bf[0:1, s * own : (s + 1) * own] = bm[s] * scb[s]

        give_before.start()

        @pl.loop(0, slots)
        def _(s):
            peak_ref[:, half_col(c, s)] = jnp.maximum(ccl[mine, cols(s)], bf[0:1, cols(s)])

        drain(ratio_ref.at[:, other_half], or_r.at[0])
        drain(peak_ref.at[:, other_half], op_r.at[0])
        give_before.wait_recv()

        @pl.loop(0, slots)
        def _(s):
            other = half_col(1 - c, s)
            peak_ref[:, other] = jnp.maximum(peak_ref[:, other], bo[0:1, cols(s)])

        give_before.wait_send()
        drain(ratio_ref.at[:, other_half], or_s.at[0])
        drain(peak_ref.at[:, other_half], op_s.at[0])

        @pl.loop(q - hist + 1, late)
        def _(k):
            drain(mrow, mx_s.at[k])

        drain(scb.at[pl.ds(0, late - 1)], sc_s.at[0])
        drain(cb.at[pl.ds(0, hist - 1)], cb_s.at[0])

    swap_v.wait_send()
    swap_w.wait_send()

    @pl.when(is_hist)
    def _():
        drain(ow.at[pl.ds(0, (2 * hist - 1) * rows), :], ow_s.at[0])
        drain(tb.at[pl.ds(0, hist - 1)], tp_s.at[0])
        drain(cb, cb_s.at[0])
        give_count.wait_send()
        drain(sq, sq_s.at[0])

    @pl.when(totals)
    def _():
        send_total.wait_send()

    @pl.when(sends_early)
    def _():
        drain(w_ref, hw_s.at[0])
        drain(v_ref, ha_s.at[0])

    @pl.when(late_passes)
    def _():
        drain(fw, fw_s.at[0])

    @pl.when(forwards)
    def _():
        drain(hv.at[:, pl.ds(direct * own, (later - direct) * own)], fw_s.at[0])


def store_kernel(ratio_ref, peak_ref, ratio_hbm, peak_hbm, sems):
    copies = [
        pltpu.make_async_copy(ratio_ref, ratio_hbm, sems.at[0]),
        pltpu.make_async_copy(peak_ref, peak_hbm, sems.at[1]),
    ]
    for copy in copies:
        copy.start()
    for copy in copies:
        copy.wait()


def fused_device(narrow, devices, values, cloud_words, history_len, monitor_start, boundary_table):
    rows, pixels = values.shape
    chips, chip_rows, half = devices // 2, 2 * rows, pixels // 2
    dates = boundary_table.shape[0]
    hist, back = HISTORY_MOST // chip_rows, WINDOW // chip_rows
    own, late = half // hist, chips - hist
    design = host_design(dates)
    lower = [(i, j) for i in range(COLS) for j in range(i + 1)]
    outer = np.zeros((40, HISTORY_MOST), np.float32)
    for at, (i, j) in enumerate(lower):
        outer[at] = design[:HISTORY_MOST, i] * design[:HISTORY_MOST, j]
    by_chip = design.reshape(chips, chip_rows, COLS)
    hbm = pl.BlockSpec(memory_space=pltpu.HBM)
    f32, i32, dma = jnp.float32, jnp.int32, pltpu.SemaphoreType.DMA
    scratch = [
        pltpu.SMEM((1,), i32),
        pltpu.SMEM((1,), i32),
        pltpu.SMEM((dates,), i32),
        pltpu.VMEM((rows, pixels), f32),
        pltpu.VMEM((rows, pixels // 32), i32),
        pltpu.VMEM((chip_rows, own), f32),
        pltpu.VMEM((chip_rows, half), f32),
        pltpu.VMEM((chip_rows, pixels // 32), i32),
        pltpu.VMEM((chip_rows, half), f32),
        pltpu.VMEM((chip_rows, half), f32),
        pltpu.VMEM((chip_rows, pixels // 32), i32),
        pltpu.VMEM((HISTORY_MOST, 128), i32),
        pltpu.VMEM((hist, COLS, own), f32),
        pltpu.VMEM((hist, COLS, own), f32),
        pltpu.VMEM((40, own), f32),
        pltpu.VMEM((hist, COLS, own), f32),
        pltpu.VMEM((1, own), f32),
        pltpu.VMEM((hist, 1, own), f32),
        pltpu.VMEM((hist, 1, own), f32),
        pltpu.VMEM((1, half), f32),
        pltpu.VMEM((1, half), f32),
        pltpu.VMEM((1, half), f32),
        pltpu.VMEM((1, half), f32),
        pltpu.VMEM((hist, 1, own), f32),
        pltpu.VMEM((1, own), f32),
        pltpu.VMEM((late, 1, own), f32),
        pltpu.VMEM((chip_rows, half), f32),
        pltpu.VMEM((hist, 1, own), f32),
        pltpu.VMEM((late, hist, 1, own), f32),
        pltpu.VMEM((chip_rows, COLS), f32),
        pltpu.VMEM((chip_rows, COLS), f32),
        pltpu.VMEM((40, HISTORY_MOST), f32),
    ]
    scratch += [pltpu.SemaphoreType.REGULAR((1,))]
    scratch += [dma((2,)), dma((2,)), dma((1,)), dma((hist,)), dma((1,)), dma((1,))]
    for number in (1, 1, 1):
        scratch += [dma((number,)), dma((number,))]
    scratch += [dma((1,)), dma((1 + late // 2,))]
    for number in (1, 1):
        scratch += [dma((number,)), dma((number,))]
    scratch += [dma((1,)), dma((1,))]
    for number in (1, late, 1, 1, 1):
        scratch += [dma((number,)), dma((number,))]
    scratch.append(dma((11,)))
    outs = pl.pallas_call(
        functools.partial(fused_kernel, narrow, chips, hist, back),
        out_shape=[pltpu.VMEM((rows, pixels), f32)] * 2,
        in_specs=[hbm] * 7,
        scratch_shapes=scratch,
        compiler_params=pltpu.CompilerParams(
            has_side_effects=True, collective_id=0, vmem_limit_bytes=67043328 - 2 * rows * pixels * 4),
    )(
        history_len, monitor_start, boundary_table, values, cloud_words,
        jnp.asarray(by_chip), jnp.asarray(outer),
    )
    return pl.pallas_call(
        store_kernel,
        out_shape=[jax.ShapeDtypeStruct((rows, pixels), f32)] * 2,
        in_specs=[pl.BlockSpec(memory_space=pltpu.VMEM)] * 2,
        out_specs=[pl.BlockSpec(memory_space=pl.ANY)] * 2,
        scratch_shapes=[dma((2,))],
        compiler_params=pltpu.CompilerParams(vmem_limit_bytes=8 * 1024 * 1024),
    )(*outs)


def fits(narrow, devices, rows, pixels):
    chip_rows = 2 * rows
    if narrow % 2 or rows % 8 or HISTORY_MOST % chip_rows or WINDOW != 2 * chip_rows:
        return False
    hist = HISTORY_MOST // chip_rows
    return devices // 2 == 2 * hist and (pixels // 2) % (hist * 128) == 0 and 128 % (pixels // 64 // hist) == 0


def solution(mesh):
    narrow = mesh.shape["narrow"]
    devices = narrow * mesh.shape["wide"]

    def per_device_any(values, *rest):
        if fits(narrow, devices, *values.shape):
            return fused_device(narrow, devices, values, *rest)
        return per_device(values, *rest)

    placed = (P(("wide", "narrow"), None), P(("wide", "narrow"), None), P(), P(), P())
    return jax.shard_map(
        per_device_any,
        mesh=mesh,
        in_specs=placed,
        out_specs=(P(("wide", "narrow"), None), P(("wide", "narrow"), None)),
        check_vma=False,
    )
```
